32 devices in a mesh: fsdp: 32 (over z, y, x, core).
Axes of the slice: x: 2, y: 2, z: 4, core: 2. Of those that a mesh axis runs over, the one named last changes fastest.
Arguments:
- tok_ids: int32 [32768], P('fsdp')
- tok_labels: int32 [32768], P('fsdp')
- loss_mask: int32 [32768], P('fsdp')
- emb_table: bfloat16 [20480, 256], P('fsdp')
- gain_mlp: float32 [256], replicated
- gain_head: float32 [256], replicated
- w_gate: bfloat16 [256, 2048], P('fsdp')
- w_up: bfloat16 [256, 2048], P('fsdp')
- w_down: bfloat16 [2048, 256], P('fsdp')
Outputs:
- output 1: float32 [], replicated
- output 2: float32 [20480, 256], P('fsdp')
- output 3: float32 [256, 2048], P('fsdp')
- output 4: float32 [256, 2048], P('fsdp')
- output 5: float32 [2048, 256], P('fsdp')
All inputs are finite; a program needn't handle non-finite values.
Results may differ from the reference program's by a relative error of at most 0.00898581.
Values are sent between devices in bfloat16 or wider.
A program may use at most 1 GiB of HBM per device.

```python
import jax
import jax.numpy as jnp
from jax import lax

VOCAB = 20480
D_MODEL = 256
D_FF = 2048
TOK_DEV = 1024
GROUP_SIZE = 32
T_GLOBAL = TOK_DEV * GROUP_SIZE
NORM_EPS = 1e-6
ROW_CONTRACT = (((1,), (1,)), ((), ()))
TOK_CONTRACT = (((0,), (0,)), ((), ()))


def draw_tokens(tok_key):
    key_ids, key_lab, key_pad, key_cut = jax.random.split(tok_key, 4)
    tok_ids = jax.random.randint(key_ids, (T_GLOBAL,), 0, VOCAB, dtype=jnp.int32)
    tok_ids = tok_ids.at[0].set(0).at[1].set(VOCAB - 1)
    tok_labels = jax.random.randint(key_lab, (T_GLOBAL,), 0, VOCAB, dtype=jnp.int32)
    tok_labels = tok_labels.at[0].set(VOCAB - 1).at[1].set(0)
    pad_len = jax.random.randint(key_pad, (GROUP_SIZE, 1), 0, TOK_DEV // 2 + 1, dtype=jnp.int32)
    keep_tail = jnp.arange(TOK_DEV)[None, :] < TOK_DEV - pad_len
    cut_draw = jax.random.randint(key_cut, (GROUP_SIZE, TOK_DEV), 0, 16, dtype=jnp.int32)
    loss_mask = (keep_tail & (cut_draw != 0)).astype(jnp.int32).reshape(T_GLOBAL)
    return tok_ids, tok_labels, loss_mask.at[0].set(1)


def setup_inputs(seed: int = 0) -> dict:
    root_key = jax.random.key(seed)
    key_tok, key_emb, key_g1, key_g2, key_gate, key_up, key_down = jax.random.split(root_key, 7)
    tok_ids, tok_labels, loss_mask = draw_tokens(key_tok)
    emb_table = (jax.random.normal(key_emb, (VOCAB, D_MODEL), jnp.float32) * D_MODEL ** -0.5).astype(jnp.bfloat16)
    gain_mlp = 1.0 + 0.5 * jax.random.normal(key_g1, (D_MODEL,), jnp.float32)
    gain_head = 1.0 + 0.5 * jax.random.normal(key_g2, (D_MODEL,), jnp.float32)
    w_gate = (jax.random.normal(key_gate, (D_MODEL, D_FF), jnp.float32) * D_MODEL ** -0.5).astype(jnp.bfloat16)
    w_up = (jax.random.normal(key_up, (D_MODEL, D_FF), jnp.float32) * D_MODEL ** -0.5).astype(jnp.bfloat16)
    w_down = (jax.random.normal(key_down, (D_FF, D_MODEL), jnp.float32) * 1.5 * (D_FF * D_MODEL) ** -0.5).astype(jnp.bfloat16)
    return {"tok_ids": tok_ids, "tok_labels": tok_labels, "loss_mask": loss_mask, "emb_table": emb_table, "gain_mlp": gain_mlp, "gain_head": gain_head, "w_gate": w_gate, "w_up": w_up, "w_down": w_down}


def rms_scale(rows_wide, norm_gain):
    inv_rms = lax.rsqrt(jnp.mean(rows_wide * rows_wide, axis=-1, keepdims=True) + NORM_EPS)
    return (rows_wide * inv_rms * norm_gain).astype(jnp.bfloat16), inv_rms


def rms_back(rows_wide, inv_rms, norm_gain, grad_out):
    scaled_grad = grad_out * norm_gain
    return inv_rms * (scaled_grad - rows_wide * (inv_rms * inv_rms) * jnp.mean(scaled_grad * rows_wide, axis=-1, keepdims=True))


def mlp_forward(emb_rows, gain_mlp, gain_head, w_gate, w_up, w_down):
    emb_wide = emb_rows.astype(jnp.float32)
    a_norm, inv_first = rms_scale(emb_wide, gain_mlp)
    gate_wide = jnp.dot(a_norm, w_gate, preferred_element_type=jnp.float32).astype(jnp.bfloat16).astype(jnp.float32)
    up_wide = jnp.dot(a_norm, w_up, preferred_element_type=jnp.float32).astype(jnp.bfloat16).astype(jnp.float32)
    gate_sig = jax.nn.sigmoid(gate_wide)
    act_rows = (gate_wide * gate_sig * up_wide).astype(jnp.bfloat16)
    hid_wide = (emb_wide + jnp.dot(act_rows, w_down, preferred_element_type=jnp.float32)).astype(jnp.bfloat16).astype(jnp.float32)
    h_norm, inv_second = rms_scale(hid_wide, gain_head)
    return (emb_wide, inv_first, a_norm, gate_wide, up_wide, gate_sig, act_rows, hid_wide, inv_second), h_norm


def head_forward(h_norm, emb_table, tok_labels, tok_coef):
    logits = lax.dot_general(h_norm, emb_table, ROW_CONTRACT, preferred_element_type=jnp.float32)
    row_max = jnp.max(logits, axis=-1, keepdims=True)
    exp_rows = jnp.exp(logits - row_max)
    sum_exp = jnp.sum(exp_rows, axis=-1, keepdims=True)
    is_label = jnp.arange(logits.shape[1])[None, :] == tok_labels[:, None]
    picked = jnp.sum(jnp.where(is_label, logits, 0.0), axis=-1)
    tok_loss = row_max[:, 0] + jnp.log(sum_exp[:, 0]) - picked
    d_logits = ((exp_rows / sum_exp - is_label.astype(jnp.float32)) * tok_coef[:, None]).astype(jnp.bfloat16)
    return jnp.sum(tok_coef * tok_loss), d_logits


def mlp_backward(saved, d_hidden, gain_mlp, w_gate, w_up, w_down):
    emb_wide, inv_first, a_norm, gate_wide, up_wide, gate_sig, act_rows = saved[:7]
    hid_grad = d_hidden.astype(jnp.bfloat16)
    d_act = lax.dot_general(hid_grad, w_down, ROW_CONTRACT, preferred_element_type=jnp.float32)
    grad_down = lax.dot_general(act_rows, hid_grad, TOK_CONTRACT, preferred_element_type=jnp.float32)
    d_up = (d_act * gate_wide * gate_sig).astype(jnp.bfloat16)
    d_gate = (d_act * up_wide * gate_sig * (1.0 + gate_wide * (1.0 - gate_sig))).astype(jnp.bfloat16)
    grad_gate = lax.dot_general(a_norm, d_gate, TOK_CONTRACT, preferred_element_type=jnp.float32)
    grad_up = lax.dot_general(a_norm, d_up, TOK_CONTRACT, preferred_element_type=jnp.float32)
    d_anorm = lax.dot_general(d_gate, w_gate, ROW_CONTRACT, preferred_element_type=jnp.float32) + lax.dot_general(d_up, w_up, ROW_CONTRACT, preferred_element_type=jnp.float32)
    grad_x = d_hidden + rms_back(emb_wide, inv_first, gain_mlp, d_anorm)
    return grad_x, grad_gate, grad_up, grad_down


def block_grads(tok_ids, tok_labels, tok_coef, emb_table, gain_mlp, gain_head, w_gate, w_up, w_down):
    saved, h_norm = mlp_forward(jnp.take(emb_table, tok_ids, axis=0), gain_mlp, gain_head, w_gate, w_up, w_down)
    loss_part, d_logits = head_forward(h_norm, emb_table, tok_labels, tok_coef)
    d_hnorm = jnp.dot(d_logits, emb_table, preferred_element_type=jnp.float32)
    head_grad = lax.dot_general(d_logits, h_norm, TOK_CONTRACT, preferred_element_type=jnp.float32)
    d_hidden = rms_back(saved[7], saved[8], gain_head, d_hnorm)
    grad_x, grad_gate, grad_up, grad_down = mlp_backward(saved, d_hidden, gain_mlp, w_gate, w_up, w_down)
    grad_table = head_grad + jax.ops.segment_sum(grad_x, tok_ids, num_segments=emb_table.shape[0])
    return loss_part, grad_table, grad_gate, grad_up, grad_down


def reference(tok_ids, tok_labels, loss_mask, emb_table, gain_mlp, gain_head, w_gate, w_up, w_down):
    mask_wide = loss_mask.astype(jnp.float32)
    tok_coef = (mask_wide / jnp.sum(mask_wide)).reshape(GROUP_SIZE, TOK_DEV)

    def scan_step(acc_state, block_in):
        step_out = block_grads(block_in[0], block_in[1], block_in[2], emb_table, gain_mlp, gain_head, w_gate, w_up, w_down)
        return tuple(prev_val + new_val for prev_val, new_val in zip(acc_state, step_out)), None

    init_state = (jnp.zeros((), jnp.float32), jnp.zeros((VOCAB, D_MODEL), jnp.float32), jnp.zeros((D_MODEL, D_FF), jnp.float32), jnp.zeros((D_MODEL, D_FF), jnp.float32), jnp.zeros((D_FF, D_MODEL), jnp.float32))
    blocks = (tok_ids.reshape(GROUP_SIZE, TOK_DEV), tok_labels.reshape(GROUP_SIZE, TOK_DEV), tok_coef)
    final_state, _ = lax.scan(scan_step, init_state, blocks)
    loss_val, grad_table, grad_gate, grad_up, grad_down = final_state
    return (loss_val, grad_table, grad_gate, grad_up, grad_down)
```

```python
import functools

import jax
import jax.numpy as jnp
from jax import lax
from jax.experimental import pallas as pl
from jax.experimental.pallas import tpu as pltpu
from jax.sharding import PartitionSpec as P

NORM_EPS = 1e-6
ROW_CONTRACT = (((1,), (1,)), ((), ()))
TOK_CONTRACT = (((0,), (0,)), ((), ()))
MESH = pl.DeviceIdType.MESH
N_DEV = 32
E_ROWS = 640
W_ROWS = 192
SPLIT = 416
CHUNK = 64
HALF = CHUNK // 2
E_CHUNKS = E_ROWS // CHUNK
N_CHUNKS = (E_ROWS + W_ROWS) // CHUNK
LAG = 2
PIECES = 4
ORDER = (3, 0, 1, 2)


def dev_index(z, y, x, c):
    return z * 8 + y * 4 + x * 2 + c


def my_coords():
    me = lax.axis_index("fsdp")
    return me // 8, (me // 4) % 2, (me // 2) % 2, me % 2


def z_partners(z):
    return (z + 1 - 2 * (z % 2), (z + 2) % 4, 3 - z)


def greet(z, y, x, c):
    barrier = pltpu.get_barrier_semaphore()
    partners = [dev_index(z, y, x, 1 - c), dev_index(z, y, 1 - x, c), dev_index(z, 1 - y, x, c)]
    partners += [dev_index(zp, y, x, c) for zp in z_partners(z)]
    for dev in partners:
        pl.semaphore_signal(barrier, inc=1, device_id=(dev,), device_id_type=MESH)
    pl.semaphore_wait(barrier, 6)


def gather_kernel(e_ref, w_ref, m_ref, eo_ref, wo_ref, n_ref, tiles, send_sem, recv_sem, own_sem):
    z, y, x, c = my_coords()
    me = dev_index(z, y, x, c)
    zs = (z,) + z_partners(z)
    greet(z, y, x, c)

    own_src = (e_ref.at[pl.ds(0, SPLIT)], e_ref.at[pl.ds(SPLIT, E_ROWS - SPLIT)], w_ref, m_ref)

    def place(piece, block):
        if piece == 0:
            return eo_ref.at[block, pl.ds(0, SPLIT)]
        if piece == 1:
            return eo_ref.at[block, pl.ds(SPLIT, E_ROWS - SPLIT)]
        if piece == 2:
            return wo_ref.at[block]
        return tiles.at[block]

    sent = []
    counts = [0] * PIECES

    def send(piece, block, target, own=False):
        src = own_src[piece] if own else place(piece, block)
        copy = pltpu.make_async_remote_copy(src_ref=src, dst_ref=place(piece, block), send_sem=send_sem.at[piece, counts[piece]], recv_sem=recv_sem.at[piece, block], device_id=(target,), device_id_type=MESH)
        counts[piece] += 1
        copy.start()
        sent.append(copy)

    def arrive(piece, block):
        ref = place(piece, block)
        pltpu.make_async_copy(ref, ref, recv_sem.at[piece, block]).wait()

    to_core = dev_index(z, y, x, 1 - c)
    to_x = dev_index(z, y, 1 - x, c)
    to_y = dev_index(z, 1 - y, x, c)
    hops = ((to_y, to_x), (to_x, to_y), (to_x, to_y), (to_y, to_x))

    def block_at(piece, depth, k, j=0):
        if piece in (0, 3):
            ys, xs = ((y, x), (1 - y, x), ((y, 1 - y)[j], 1 - x))[depth]
        else:
            ys, xs = ((y, x), (y, 1 - x), (1 - y, (x, 1 - x)[j]))[depth]
        return dev_index(zs[k], ys, xs, c)

    for k in (1, 2, 3):
        for piece in ORDER:
            send(piece, me, dev_index(zs[k], y, x, c), own=True)
    for piece in ORDER:
        send(piece, me, hops[piece][0], own=True)
    for piece in ORDER:
        send(piece, me, hops[piece][1], own=True)
    for piece in ORDER:
        send(piece, me, to_core, own=True)
    keep = [pltpu.make_async_copy(own_src[piece], place(piece, me), own_sem.at[piece]) for piece in ORDER]
    for copy in keep:
        copy.start()

    for step in range(6):
        if 1 <= step < 4:
            for piece in ORDER:
                block = block_at(piece, 0, step)
                arrive(piece, block)
                send(piece, block, hops[piece][0])
                send(piece, block, hops[piece][1])
                send(piece, block, to_core)
        if 1 <= step < 5:
            for piece in ORDER:
                block = block_at(piece, 1, step - 1)
                arrive(piece, block)
                send(piece, block, hops[piece][1])
                send(piece, block, to_core)
        if 2 <= step < 6:
            for j in range(2):
                for piece in ORDER:
                    block = block_at(piece, 2, step - 2, j)
                    arrive(piece, block)
                    send(piece, block, to_core)
    for zb in range(4):
        for yb in range(2):
            for xb in range(2):
                for piece in ORDER:
                    arrive(piece, dev_index(zb, yb, xb, 1 - c))
    for copy in sent:
        copy.wait_send()
    for copy in keep:
        copy.wait()

    def total(i, acc):
        return acc + tiles[i]

    n_ref[...] = lax.fori_loop(0, N_DEV, total, jnp.zeros_like(n_ref))


def gather_all(e_shard, w_shard, mask_tile):
    vmem = pl.BlockSpec(memory_space=pltpu.VMEM)
    anyspace = pl.BlockSpec(memory_space=pl.ANY)
    return pl.pallas_call(
        gather_kernel,
        out_shape=(jax.ShapeDtypeStruct((N_DEV, E_ROWS, 256), jnp.bfloat16), jax.ShapeDtypeStruct((N_DEV, W_ROWS, 256), jnp.bfloat16), jax.ShapeDtypeStruct((8, 128), jnp.float32)),
        in_specs=[vmem, vmem, vmem],
        out_specs=(anyspace, anyspace, vmem),
        scratch_shapes=[
            pltpu.VMEM((N_DEV, 8, 128), jnp.float32),
            pltpu.SemaphoreType.DMA((PIECES, N_DEV)),
            pltpu.SemaphoreType.DMA((PIECES, N_DEV)),
            pltpu.SemaphoreType.DMA((PIECES,)),
        ],
        compiler_params=pltpu.CompilerParams(collective_id=0, has_side_effects=True),
        name="gather_all",
    )(e_shard, w_shard, mask_tile)


def scatter_kernel(g_ref, gw_ref, l_ref, out_ref, loss_ref, acc, r0, r1a, r1b, r2, r3, bufs, own_sem, s0, q0, s1, q1, s2, q2, s3, q3, small_send, small_recv):
    z, y, x, c = my_coords()
    to_core = dev_index(z, y, x, 1 - c)
    to_x = dev_index(z, y, 1 - x, c)
    to_y = dev_index(z, 1 - y, x, c)
    zs = z_partners(z)
    greet(z, y, x, c)

    def source(k, core, from_w):
        if from_w:
            return gw_ref.at[:, :, :, core, pl.ds((k - E_CHUNKS) * CHUNK, CHUNK)]
        return g_ref.at[:, :, :, core, pl.ds(k * CHUNK, CHUNK)]

    def remote(src, dst, send_sem, recv_sem, dev):
        return pltpu.make_async_remote_copy(src_ref=src, dst_ref=dst, send_sem=send_sem, recv_sem=recv_sem, device_id=(dev,), device_id_type=MESH)

    def core_away(k, src):
        return remote(src, r0.at[k], s0.at[k], q0.at[k], to_core)

    def core_mine(k, src):
        return pltpu.make_async_copy(src, acc.at[k], own_sem.at[k])

    def plane_first(k):
        return (
            remote(acc.at[k, :, :, 1 - x, pl.ds(0, HALF)], r1a.at[k], s1.at[0, k], q1.at[0, k], to_x),
            remote(acc.at[k, :, 1 - y, :, pl.ds(HALF, HALF)], r1b.at[k], s1.at[1, k], q1.at[1, k], to_y),
        )

    def plane_second(k):
        return (
            remote(r1a.at[k, :, 1 - y], r2.at[k, :, pl.ds(0, HALF)], s2.at[0, k], q2.at[0, k], to_y),
            remote(r1b.at[k, :, 1 - x], r2.at[k, :, pl.ds(HALF, HALF)], s2.at[1, k], q2.at[1, k], to_x),
        )

    def along_z(k):
        return tuple(remote(r2.at[k, zs[i]], r3.at[k, i], s3.at[i, k], q3.at[i, k], dev_index(zs[i], y, x, c)) for i in range(3))

    def begin(from_w):
        def body(k, carry):
            core_away(k, source(k, 1 - c, from_w)).start()
            core_mine(k, source(k, c, from_w)).start()
            return carry

        return body

    def small(src, slot, dev):
        return remote(src, bufs.at[slot], small_send.at[slot], small_recv.at[slot], dev)

    small_steps = (
        (small(l_ref, 0, to_core),),
        (small(bufs.at[6], 1, to_x),),
        (small(bufs.at[7], 2, to_y),),
        tuple(small(bufs.at[8], 3 + i, dev_index(zs[i], y, x, c)) for i in range(3)),
    )
    small_steps[0][0].start()
    lax.fori_loop(0, E_CHUNKS, begin(False), 0)
    lax.fori_loop(E_CHUNKS, N_CHUNKS, begin(True), 0)

    def step_body(s, carry):
        @pl.when(s < N_CHUNKS)
        def _():
            core_mine(s, acc.at[s]).wait()
            core_away(s, r0.at[s]).wait_recv()

            def add(i, inner):
                acc[s, i // 4, (i // 2) % 2, i % 2] += r0[s, i // 4, (i // 2) % 2, i % 2]
                return inner

            lax.fori_loop(0, 16, add, 0)
            for copy in plane_first(s):
                copy.start()

        @pl.when((s >= LAG) & (s < N_CHUNKS + LAG))
        def _():
            k = s - LAG
            for copy in plane_first(k):
                copy.wait_recv()

            def add(i, inner):
                r1a[k, i // 2, i % 2] += acc[k, i // 2, i % 2, x, pl.ds(0, HALF)]
                r1b[k, i // 2, i % 2] += acc[k, i // 2, y, i % 2, pl.ds(HALF, HALF)]
                return inner

            lax.fori_loop(0, 8, add, 0)
            for copy in plane_second(k):
                copy.start()

        @pl.when((s >= 2 * LAG) & (s < N_CHUNKS + 2 * LAG))
        def _():
            k = s - 2 * LAG
            for copy in plane_second(k):
                copy.wait_recv()

            def add(i, inner):
                r2[k, i, pl.ds(0, HALF)] += r1a[k, i, y]
                r2[k, i, pl.ds(HALF, HALF)] += r1b[k, i, x]
                return inner

            lax.fori_loop(0, 4, add, 0)
            for copy in along_z(k):
                copy.start()

        @pl.when(s >= 3 * LAG)
        def _():
            k = s - 3 * LAG
            for copy in along_z(k):
                copy.wait_recv()
            out_ref[k] = (r2[k, z] + r3[k, 0]) + (r3[k, 1] + r3[k, 2])

        for i in range(3):

            @pl.when(s == 1 + 3 * i)
            def _():
                small_steps[i][0].wait()
                bufs[6 + i] = (l_ref[...] if i == 0 else bufs[5 + i]) + bufs[i]
                for copy in small_steps[i + 1]:
                    copy.start()

        return carry

    lax.fori_loop(0, N_CHUNKS + 3 * LAG, step_body, 0)

    for copy in small_steps[3]:
        copy.wait()
    loss_ref[...] = (bufs[8] + bufs[3]) + (bufs[4] + bufs[5])

    def finish(k, carry):
        core_away(k, r0.at[k]).wait_send()
        for copy in plane_first(k) + plane_second(k) + along_z(k):
            copy.wait_send()
        return carry

    lax.fori_loop(0, N_CHUNKS, finish, 0)


def scatter_all(grad_blocks, weight_blocks, loss_tile):
    vmem = pl.BlockSpec(memory_space=pltpu.VMEM)
    anyspace = pl.BlockSpec(memory_space=pl.ANY)
    dma = pltpu.SemaphoreType.DMA
    return pl.pallas_call(
        scatter_kernel,
        out_shape=(jax.ShapeDtypeStruct((N_CHUNKS, CHUNK, 256), jnp.float32), jax.ShapeDtypeStruct((8, 128), jnp.float32)),
        in_specs=[anyspace, anyspace, vmem],
        out_specs=(vmem, vmem),
        scratch_shapes=[
            pltpu.VMEM((N_CHUNKS, 4, 2, 2, CHUNK, 256), jnp.float32),
            pltpu.VMEM((N_CHUNKS, 4, 2, 2, CHUNK, 256), jnp.float32),
            pltpu.VMEM((N_CHUNKS, 4, 2, HALF, 256), jnp.float32),
            pltpu.VMEM((N_CHUNKS, 4, 2, HALF, 256), jnp.float32),
            pltpu.VMEM((N_CHUNKS, 4, CHUNK, 256), jnp.float32),
            pltpu.VMEM((N_CHUNKS, 3, CHUNK, 256), jnp.float32),
            pltpu.VMEM((9, 8, 128), jnp.float32),
            dma((N_CHUNKS,)),
            dma((N_CHUNKS,)),
            dma((N_CHUNKS,)),
            dma((2, N_CHUNKS)),
            dma((2, N_CHUNKS)),
            dma((2, N_CHUNKS)),
            dma((2, N_CHUNKS)),
            dma((3, N_CHUNKS)),
            dma((3, N_CHUNKS)),
            dma((6,)),
            dma((6,)),
        ],
        compiler_params=pltpu.CompilerParams(collective_id=1, has_side_effects=True, vmem_limit_bytes=60 * 1024 * 1024),
        name="scatter_all",
    )(grad_blocks, weight_blocks, loss_tile)


def rms_scale(rows_wide, norm_gain):
    inv_rms = lax.rsqrt(jnp.mean(rows_wide * rows_wide, axis=-1, keepdims=True) + NORM_EPS)
    return (rows_wide * inv_rms * norm_gain).astype(jnp.bfloat16), inv_rms


def rms_back(rows_wide, inv_rms, norm_gain, grad_out):
    scaled_grad = grad_out * norm_gain
    return inv_rms * (scaled_grad - rows_wide * (inv_rms * inv_rms) * jnp.mean(scaled_grad * rows_wide, axis=-1, keepdims=True))


def mlp_forward(emb_rows, gain_mlp, gain_head, w_gate, w_up, w_down):
    emb_wide = emb_rows.astype(jnp.float32)
    a_norm, inv_first = rms_scale(emb_wide, gain_mlp)
    gate_wide = jnp.dot(a_norm, w_gate, preferred_element_type=jnp.float32).astype(jnp.bfloat16).astype(jnp.float32)
    up_wide = jnp.dot(a_norm, w_up, preferred_element_type=jnp.float32).astype(jnp.bfloat16).astype(jnp.float32)
    gate_sig = jax.nn.sigmoid(gate_wide)
    act_rows = (gate_wide * gate_sig * up_wide).astype(jnp.bfloat16)
    hid_wide = (emb_wide + jnp.dot(act_rows, w_down, preferred_element_type=jnp.float32)).astype(jnp.bfloat16).astype(jnp.float32)
    h_norm, inv_second = rms_scale(hid_wide, gain_head)
    return (emb_wide, inv_first, a_norm, gate_wide, up_wide, gate_sig, act_rows, hid_wide, inv_second), h_norm


def head_forward(h_norm, emb_table, tok_labels, tok_coef):
    logits = lax.dot_general(h_norm, emb_table, ROW_CONTRACT, preferred_element_type=jnp.float32)
    row_max = jnp.max(logits, axis=-1, keepdims=True)
    exp_rows = jnp.exp(logits - row_max)
    sum_exp = jnp.sum(exp_rows, axis=-1, keepdims=True)
    is_label = jnp.arange(logits.shape[1])[None, :] == tok_labels[:, None]
    picked = jnp.sum(jnp.where(is_label, logits, 0.0), axis=-1)
    tok_loss = row_max[:, 0] + jnp.log(sum_exp[:, 0]) - picked
    d_logits = ((exp_rows / sum_exp - is_label.astype(jnp.float32)) * tok_coef[:, None]).astype(jnp.bfloat16)
    return jnp.sum(tok_coef * tok_loss), d_logits


def mlp_backward(saved, d_hidden, gain_mlp, w_gate, w_up, w_down):
    emb_wide, inv_first, a_norm, gate_wide, up_wide, gate_sig, act_rows = saved[:7]
    hid_grad = d_hidden.astype(jnp.bfloat16)
    d_act = lax.dot_general(hid_grad, w_down, ROW_CONTRACT, preferred_element_type=jnp.float32)
    grad_down = lax.dot_general(act_rows, hid_grad, TOK_CONTRACT, preferred_element_type=jnp.float32)
    d_up = (d_act * gate_wide * gate_sig).astype(jnp.bfloat16)
    d_gate = (d_act * up_wide * gate_sig * (1.0 + gate_wide * (1.0 - gate_sig))).astype(jnp.bfloat16)
    grad_gate = lax.dot_general(a_norm, d_gate, TOK_CONTRACT, preferred_element_type=jnp.float32)
    grad_up = lax.dot_general(a_norm, d_up, TOK_CONTRACT, preferred_element_type=jnp.float32)
    d_anorm = lax.dot_general(d_gate, w_gate, ROW_CONTRACT, preferred_element_type=jnp.float32) + lax.dot_general(d_up, w_up, ROW_CONTRACT, preferred_element_type=jnp.float32)
    grad_x = d_hidden + rms_back(emb_wide, inv_first, gain_mlp, d_anorm)
    return grad_x, grad_gate, grad_up, grad_down


def rows_to_tiles(rows):
    return rows.reshape(-1, 8, 8, 256).transpose(0, 2, 1, 3).reshape(-1, 64, 256)


def tiles_to_rows(tiles):
    return tiles.reshape(-1, 8, 8, 256).transpose(0, 2, 1, 3).reshape(-1, 2048)


def solution(mesh):
    def device_step(tok_ids, tok_labels, loss_mask, table_shard, gain_mlp, gain_head, gate_shard, up_shard, down_shard):
        mask_wide = loss_mask.astype(jnp.float32)
        w_shard = jnp.concatenate([rows_to_tiles(gate_shard)[0], rows_to_tiles(up_shard)[0], down_shard], axis=0)
        table_blocks, w_blocks, mask_total = gather_all(table_shard, w_shard, jnp.broadcast_to(jnp.sum(mask_wide), (8, 128)))
        tok_coef = mask_wide / mask_total[0, 0]
        table_full = table_blocks.reshape(-1, 256)
        gate_full = tiles_to_rows(w_blocks[:, 0:64])
        up_full = tiles_to_rows(w_blocks[:, 64:128])
        down_full = w_blocks[:, 128:192].reshape(-1, 256)
        emb_rows = jnp.take(table_full, tok_ids, axis=0)
        saved, h_norm = mlp_forward(emb_rows, gain_mlp, gain_head, gate_full, up_full, down_full)
        loss_part, d_logits = head_forward(h_norm, table_full, tok_labels, tok_coef)
        d_hnorm = jnp.dot(d_logits, table_full, preferred_element_type=jnp.float32)
        head_grad = lax.dot_general(d_logits, h_norm, TOK_CONTRACT, preferred_element_type=jnp.float32)
        d_hidden = rms_back(saved[7], saved[8], gain_head, d_hnorm)
        grad_x, grad_gate, grad_up, grad_down = mlp_backward(saved, d_hidden, gain_mlp, gate_full, up_full, down_full)
        grad_table = head_grad + jax.ops.segment_sum(grad_x, tok_ids, num_segments=table_full.shape[0])
        grad_w = jnp.concatenate([rows_to_tiles(grad_gate), rows_to_tiles(grad_up), grad_down.reshape(-1, 64, 256)], axis=1)
        out, loss = scatter_all(grad_table.reshape(4, 2, 2, 2, E_ROWS, 256), grad_w.reshape(4, 2, 2, 2, W_ROWS, 256), jnp.broadcast_to(loss_part, (8, 128)))
        g_tab = out[:E_CHUNKS].reshape(E_ROWS, 256)
        return loss[0, 0], g_tab, tiles_to_rows(out[E_CHUNKS]), tiles_to_rows(out[E_CHUNKS + 1]), out[E_CHUNKS + 2]

    row_spec = P("fsdp", None)
    tok_spec = P("fsdp")
    return jax.shard_map(device_step, mesh=mesh, in_specs=(tok_spec, tok_spec, tok_spec, row_spec, P(), P(), row_spec, row_spec, row_spec), out_specs=(P(), row_spec, row_spec, row_spec, row_spec), check_vma=False)
```

```python
import functools

import jax
import jax.numpy as jnp
from jax import lax
from jax.experimental import pallas as pl
from jax.experimental.pallas import tpu as pltpu
from jax.sharding import PartitionSpec as P

NORM_EPS = 1e-6
ROW_CONTRACT = (((1,), (1,)), ((), ()))
TOK_CONTRACT = (((0,), (0,)), ((), ()))
MESH = pl.DeviceIdType.MESH
N_DEV = 32
E_ROWS = 640
W_ROWS = 192
SPLIT = 416
CHUNK = 64
HALF = CHUNK // 2
E_CHUNKS = E_ROWS // CHUNK
N_CHUNKS = (E_ROWS + W_ROWS) // CHUNK
LAG = 2
AHEAD = 2
W_CHUNKS = 3
LOG2E = 1.4426950408889634
LN2 = 0.6931471805599453
VOCAB_TILE = 2048
UNIT = 512
TOK_TILE = 256
PIECES = 4
ORDER = (3, 0, 1, 2)


def dev_index(z, y, x, c):
    return z * 8 + y * 4 + x * 2 + c


def my_coords():
    me = lax.axis_index("fsdp")
    return me // 8, (me // 4) % 2, (me // 2) % 2, me % 2


def z_partners(z):
    return (z + 1 - 2 * (z % 2), (z + 2) % 4, 3 - z)


def greet(z, y, x, c):
    barrier = pltpu.get_barrier_semaphore()
    partners = [dev_index(z, y, x, 1 - c), dev_index(z, y, 1 - x, c), dev_index(z, 1 - y, x, c)]
    partners += [dev_index(zp, y, x, c) for zp in z_partners(z)]
    for dev in partners:
        pl.semaphore_signal(barrier, inc=1, device_id=(dev,), device_id_type=MESH)
    pl.semaphore_wait(barrier, 6)


def gather_kernel(e_ref, w_ref, m_ref, eo_ref, wo_ref, n_ref, tiles, send_sem, recv_sem, own_sem):
    z, y, x, c = my_coords()
    me = dev_index(z, y, x, c)
    zs = (z,) + z_partners(z)
    greet(z, y, x, c)

    own_src = (e_ref.at[pl.ds(0, SPLIT)], e_ref.at[pl.ds(SPLIT, E_ROWS - SPLIT)], w_ref, m_ref)

    def place(piece, block):
        if piece == 0:
            return eo_ref.at[block, pl.ds(0, SPLIT)]
        if piece == 1:
            return eo_ref.at[block, pl.ds(SPLIT, E_ROWS - SPLIT)]
        if piece == 2:
            return wo_ref.at[block]
        return tiles.at[block]

    sent = []
    counts = [0] * PIECES

    def send(piece, block, target, own=False):
        src = own_src[piece] if own else place(piece, block)
        copy = pltpu.make_async_remote_copy(src_ref=src, dst_ref=place(piece, block), send_sem=send_sem.at[piece, counts[piece]], recv_sem=recv_sem.at[piece, block], device_id=(target,), device_id_type=MESH)
        counts[piece] += 1
        copy.start()
        sent.append(copy)

    def arrive(piece, block):
        ref = place(piece, block)
        pltpu.make_async_copy(ref, ref, recv_sem.at[piece, block]).wait()

    to_core = dev_index(z, y, x, 1 - c)
    to_x = dev_index(z, y, 1 - x, c)
    to_y = dev_index(z, 1 - y, x, c)
    hops = ((to_y, to_x), (to_x, to_y), (to_x, to_y), (to_y, to_x))

    def block_at(piece, depth, k, j=0):
        if piece in (0, 3):
            ys, xs = ((y, x), (1 - y, x), ((y, 1 - y)[j], 1 - x))[depth]
        else:
            ys, xs = ((y, x), (y, 1 - x), (1 - y, (x, 1 - x)[j]))[depth]
        return dev_index(zs[k], ys, xs, c)

    for k in (1, 2, 3):
        for piece in ORDER:
            send(piece, me, dev_index(zs[k], y, x, c), own=True)
    for piece in ORDER:
        send(piece, me, hops[piece][0], own=True)
    for piece in ORDER:
        send(piece, me, hops[piece][1], own=True)
    for piece in ORDER:
        send(piece, me, to_core, own=True)
    keep = [pltpu.make_async_copy(own_src[piece], place(piece, me), own_sem.at[piece]) for piece in ORDER]
    for copy in keep:
        copy.start()

    for step in range(6):
        if 1 <= step < 4:
            for piece in ORDER:
                block = block_at(piece, 0, step)
                arrive(piece, block)
                send(piece, block, hops[piece][0])
                send(piece, block, hops[piece][1])
                send(piece, block, to_core)
        if 1 <= step < 5:
            for piece in ORDER:
                block = block_at(piece, 1, step - 1)
                arrive(piece, block)
                send(piece, block, hops[piece][1])
                send(piece, block, to_core)
        if 2 <= step < 6:
            for j in range(2):
                for piece in ORDER:
                    block = block_at(piece, 2, step - 2, j)
                    arrive(piece, block)
                    send(piece, block, to_core)
    for zb in range(4):
        for yb in range(2):
            for xb in range(2):
                for piece in ORDER:
                    arrive(piece, dev_index(zb, yb, xb, 1 - c))
    for copy in sent:
        copy.wait_send()
    for copy in keep:
        copy.wait()

    def total(i, acc):
        return acc + tiles[i]

    n_ref[...] = lax.fori_loop(0, N_DEV, total, jnp.zeros_like(n_ref))


def gather_all(e_shard, w_shard, mask_tile):
    vmem = pl.BlockSpec(memory_space=pltpu.VMEM)
    anyspace = pl.BlockSpec(memory_space=pl.ANY)
    return pl.pallas_call(
        gather_kernel,
        out_shape=(jax.ShapeDtypeStruct((N_DEV, E_ROWS, 256), jnp.bfloat16), jax.ShapeDtypeStruct((N_DEV, W_ROWS, 256), jnp.bfloat16), jax.ShapeDtypeStruct((8, 128), jnp.float32)),
        in_specs=[vmem, vmem, vmem],
        out_specs=(anyspace, anyspace, vmem),
        scratch_shapes=[
            pltpu.VMEM((N_DEV, 8, 128), jnp.float32),
            pltpu.SemaphoreType.DMA((PIECES, N_DEV)),
            pltpu.SemaphoreType.DMA((PIECES, N_DEV)),
            pltpu.SemaphoreType.DMA((PIECES,)),
        ],
        compiler_params=pltpu.CompilerParams(collective_id=0, has_side_effects=True),
        name="gather_all",
    )(e_shard, w_shard, mask_tile)


def scatter_kernel(dl_ref, hn_ref, dx_ref, id_ref, gg_ref, gu_ref, gd_ref, l_ref, out_ref, loss_ref, acc, r0, r1a, r1b, r2, r3, bufs, dl_buf, away_buf, hot, own_sem, load_sem, s0, q0, s1, q1, s2, q2, s3, q3, small_send, small_recv):
    z, y, x, c = my_coords()
    to_core = dev_index(z, y, x, 1 - c)
    to_x = dev_index(z, y, 1 - x, c)
    to_y = dev_index(z, 1 - y, x, c)
    zs = z_partners(z)
    greet(z, y, x, c)

    def remote(src, dst, send_sem, recv_sem, dev):
        return pltpu.make_async_remote_copy(src_ref=src, dst_ref=dst, send_sem=send_sem, recv_sem=recv_sem, device_id=(dev,), device_id_type=MESH)

    def core_away(k, src):
        return remote(src, r0.at[k], s0.at[k], q0.at[k], to_core)

    def load(k):
        slot = k % 2
        return pltpu.make_async_copy(dl_ref.at[:, :, :, :, pl.ds((k - W_CHUNKS) * CHUNK, CHUNK)], dl_buf.at[slot], load_sem.at[slot])

    def table_rows(k):
        slot = k % 2
        load(k).wait()

        @pl.when(k >= W_CHUNKS + 2)
        def _():
            core_away(k - 2, away_buf.at[slot]).wait_send()

        row = lax.broadcasted_iota(jnp.int32, (CHUNK, id_ref.shape[1]), 0)
        hn = hn_ref[...]
        dx = dx_ref[...]
        for mine in range(2):
            core = c if mine else 1 - c

            def part(zp, carry, mine=mine, core=core):
                for i in range(8):
                    dev = dev_index(2 * zp + i // 4, (i // 2) % 2, i % 2, core)
                    here = row == id_ref[...] - (dev * E_ROWS + (k - W_CHUNKS) * CHUNK)
                    hot[i * CHUNK : (i + 1) * CHUNK] = jnp.where(here, 1.0, 0.0).astype(jnp.bfloat16)
                head = jnp.dot(dl_buf[slot, pl.ds(2 * zp, 2), :, :, core].reshape(8 * CHUNK, -1), hn, preferred_element_type=jnp.float32)
                rows = jnp.dot(hot[...], dx, preferred_element_type=jnp.float32)
                rows = rows[:, 0:256] + (rows[:, 256:512] + rows[:, 512:768])
                total = (head + 2.0 * rows).reshape(2, 2, 2, CHUNK, 256)
                if mine:
                    acc[k, pl.ds(2 * zp, 2)] = total
                else:
                    away_buf[slot, pl.ds(2 * zp, 2)] = total
                return carry

            lax.fori_loop(0, 2, part, 0)
            if not mine:
                core_away(k, away_buf.at[slot]).start()

        @pl.when(k + 2 < N_CHUNKS)
        def _():
            load(k + 2).start()

    def plane_first(k):
        return (
            remote(acc.at[k, :, :, 1 - x, pl.ds(0, HALF)], r1a.at[k], s1.at[0, k], q1.at[0, k], to_x),
            remote(acc.at[k, :, 1 - y, :, pl.ds(HALF, HALF)], r1b.at[k], s1.at[1, k], q1.at[1, k], to_y),
        )

    def plane_second(k):
        return (
            remote(r1a.at[k, :, 1 - y], r2.at[k, :, pl.ds(0, HALF)], s2.at[0, k], q2.at[0, k], to_y),
            remote(r1b.at[k, :, 1 - x], r2.at[k, :, pl.ds(HALF, HALF)], s2.at[1, k], q2.at[1, k], to_x),
        )

    def along_z(k):
        return tuple(remote(r2.at[k, zs[i]], r3.at[k, i], s3.at[i, k], q3.at[i, k], dev_index(zs[i], y, x, c)) for i in range(3))

    def small(src, slot, dev):
        return remote(src, bufs.at[slot], small_send.at[slot], small_recv.at[slot], dev)

    small_steps = (
        (small(l_ref, 0, to_core),),
        (small(bufs.at[6], 1, to_x),),
        (small(bufs.at[7], 2, to_y),),
        tuple(small(bufs.at[8], 3 + i, dev_index(zs[i], y, x, c)) for i in range(3)),
    )
    small_steps[0][0].start()
    w_refs = (gg_ref, gu_ref, gd_ref)
    for k in range(W_CHUNKS):
        core_away(k, w_refs[k].at[:, :, :, 1 - c]).start()
        pltpu.make_async_copy(w_refs[k].at[:, :, :, c], acc.at[k], own_sem.at[k]).start()
    for k in range(W_CHUNKS, W_CHUNKS + 2):
        load(k).start()

    def step_body(s, carry):
        @pl.when((s + AHEAD >= W_CHUNKS) & (s + AHEAD < N_CHUNKS))
        def _():
            table_rows(s + AHEAD)

        @pl.when(s < W_CHUNKS)
        def _():
            pltpu.make_async_copy(acc.at[s], acc.at[s], own_sem.at[s]).wait()

        @pl.when(s < N_CHUNKS)
        def _():
            core_away(s, r0.at[s]).wait_recv()

            def add(i, inner):
                acc[s, i // 4, (i // 2) % 2, i % 2] += r0[s, i // 4, (i // 2) % 2, i % 2]
                return inner

            lax.fori_loop(0, 16, add, 0)
            for copy in plane_first(s):
                copy.start()

        @pl.when((s >= LAG) & (s < N_CHUNKS + LAG))
        def _():
            k = s - LAG
            for copy in plane_first(k):
                copy.wait_recv()

            def add(i, inner):
                r1a[k, i // 2, i % 2] += acc[k, i // 2, i % 2, x, pl.ds(0, HALF)]
                r1b[k, i // 2, i % 2] += acc[k, i // 2, y, i % 2, pl.ds(HALF, HALF)]
                return inner

            lax.fori_loop(0, 8, add, 0)
            for copy in plane_second(k):
                copy.start()

        @pl.when((s >= 2 * LAG) & (s < N_CHUNKS + 2 * LAG))
        def _():
            k = s - 2 * LAG
            for copy in plane_second(k):
                copy.wait_recv()

            def add(i, inner):
                r2[k, i, pl.ds(0, HALF)] += r1a[k, i, y]
                r2[k, i, pl.ds(HALF, HALF)] += r1b[k, i, x]
                return inner

            lax.fori_loop(0, 4, add, 0)
            for copy in along_z(k):
                copy.start()

        @pl.when(s >= 3 * LAG)
        def _():
            k = s - 3 * LAG
            for copy in along_z(k):
                copy.wait_recv()
            out_ref[k] = (r2[k, z] + r3[k, 0]) + (r3[k, 1] + r3[k, 2])

        for i in range(3):

            @pl.when(s == 1 + 3 * i)
            def _():
                small_steps[i][0].wait()
                bufs[6 + i] = (l_ref[...] if i == 0 else bufs[5 + i]) + bufs[i]
                for copy in small_steps[i + 1]:
                    copy.start()

        return carry

    lax.fori_loop(0, N_CHUNKS + 3 * LAG, step_body, 0)

    for copy in small_steps[3]:
        copy.wait()
    loss_ref[...] = (bufs[8] + bufs[3]) + (bufs[4] + bufs[5])

    for k in (*range(W_CHUNKS), N_CHUNKS - 2, N_CHUNKS - 1):
        core_away(k, r0.at[k]).wait_send()

    def finish(k, carry):
        for copy in plane_first(k) + plane_second(k) + along_z(k):
            copy.wait_send()
        return carry

    lax.fori_loop(0, N_CHUNKS, finish, 0)


def scatter_all(d_logits_t, h_norm, dx_parts, tok_ids, grad_gate, grad_up, grad_down, loss_tile):
    vmem = pl.BlockSpec(memory_space=pltpu.VMEM)
    anyspace = pl.BlockSpec(memory_space=pl.ANY)
    dma = pltpu.SemaphoreType.DMA
    n_tok = h_norm.shape[0]
    mesh_rows = (4, 2, 2, 2)
    return pl.pallas_call(
        scatter_kernel,
        out_shape=(jax.ShapeDtypeStruct((N_CHUNKS, CHUNK, 256), jnp.float32), jax.ShapeDtypeStruct((8, 128), jnp.float32)),
        in_specs=[anyspace, vmem, vmem, vmem, anyspace, anyspace, anyspace, vmem],
        out_specs=(vmem, vmem),
        scratch_shapes=[
            pltpu.VMEM((N_CHUNKS, 4, 2, 2, CHUNK, 256), jnp.float32),
            pltpu.VMEM((N_CHUNKS, 4, 2, 2, CHUNK, 256), jnp.float32),
            pltpu.VMEM((N_CHUNKS, 4, 2, HALF, 256), jnp.float32),
            pltpu.VMEM((N_CHUNKS, 4, 2, HALF, 256), jnp.float32),
            pltpu.VMEM((N_CHUNKS, 4, CHUNK, 256), jnp.float32),
            pltpu.VMEM((N_CHUNKS, 3, CHUNK, 256), jnp.float32),
            pltpu.VMEM((9, 8, 128), jnp.float32),
            pltpu.VMEM((2, *mesh_rows, CHUNK, n_tok), jnp.bfloat16),
            pltpu.VMEM((2, 4, 2, 2, CHUNK, 256), jnp.float32),
            pltpu.VMEM((8 * CHUNK, n_tok), jnp.bfloat16),
            dma((W_CHUNKS,)),
            dma((2,)),
            dma((N_CHUNKS,)),
            dma((N_CHUNKS,)),
            dma((2, N_CHUNKS)),
            dma((2, N_CHUNKS)),
            dma((2, N_CHUNKS)),
            dma((2, N_CHUNKS)),
            dma((3, N_CHUNKS)),
            dma((3, N_CHUNKS)),
            dma((6,)),
            dma((6,)),
        ],
        compiler_params=pltpu.CompilerParams(collective_id=1, has_side_effects=True, vmem_limit_bytes=63 * 1024 * 1024),
        name="scatter_all",
    )(d_logits_t.reshape(*mesh_rows, E_ROWS, n_tok), h_norm, dx_parts, tok_ids, *(g.reshape(*mesh_rows, 64, 256) for g in (grad_gate, grad_up, grad_down)), loss_tile)


def rms_scale(rows_wide, norm_gain):
    inv_rms = lax.rsqrt(jnp.mean(rows_wide * rows_wide, axis=-1, keepdims=True) + NORM_EPS)
    return (rows_wide * inv_rms * norm_gain).astype(jnp.bfloat16), inv_rms


def rms_back(rows_wide, inv_rms, norm_gain, grad_out):
    scaled_grad = grad_out * norm_gain
    return inv_rms * (scaled_grad - rows_wide * (inv_rms * inv_rms) * jnp.mean(scaled_grad * rows_wide, axis=-1, keepdims=True))


def mlp_forward(emb_rows, gain_mlp, gain_head, w_gate, w_up, w_down):
    emb_wide = emb_rows.astype(jnp.float32)
    a_norm, inv_first = rms_scale(emb_wide, gain_mlp)
    gate_wide = jnp.dot(a_norm, w_gate, preferred_element_type=jnp.float32).astype(jnp.bfloat16).astype(jnp.float32)
    up_wide = jnp.dot(a_norm, w_up, preferred_element_type=jnp.float32).astype(jnp.bfloat16).astype(jnp.float32)
    gate_sig = jax.nn.sigmoid(gate_wide)
    act_rows = (gate_wide * gate_sig * up_wide).astype(jnp.bfloat16)
    hid_wide = (emb_wide + jnp.dot(act_rows, w_down, preferred_element_type=jnp.float32)).astype(jnp.bfloat16).astype(jnp.float32)
    h_norm, inv_second = rms_scale(hid_wide, gain_head)
    return (emb_wide, inv_first, a_norm, gate_wide, up_wide, gate_sig, act_rows, hid_wide, inv_second), h_norm


def head_kernel(ht_ref, e_ref, lab_ref, coef_ref, dl_ref, dhn_ref, loss_ref, m_s, s_s, pick_s, bias_s):
    phase, j = pl.program_id(0), pl.program_id(1)
    n_tok = ht_ref.shape[1]
    n_tiles = pl.num_programs(1)
    vt, ur, tb = VOCAB_TILE, UNIT, TOK_TILE
    units = [(b, r) for b in range(n_tok // tb) for r in range(vt // ur)]

    def scaled(unit):
        b, r = unit
        return jnp.dot(e_ref[r * ur : (r + 1) * ur], ht_ref[:, b * tb : (b + 1) * tb], preferred_element_type=jnp.float32)

    def pipeline(process):
        ahead = scaled(units[0])
        for i, unit in enumerate(units):
            now = ahead
            if i + 1 < len(units):
                ahead = scaled(units[i + 1])
            process(unit, now.reshape(ur // 8, 8, tb))

    @pl.when(phase == 0)
    def _():
        @pl.when(j == 0)
        def _():
            m_s[...] = jnp.full_like(m_s, -jnp.inf)
            s_s[...] = jnp.zeros_like(s_s)
            pick_s[...] = jnp.zeros_like(pick_s)

        def process(unit, t):
            cols = pl.ds(unit[0] * tb, tb)
            m_old = m_s[:, cols]
            m_new = jnp.maximum(m_old, jnp.max(t, axis=0))
            m_s[:, cols] = m_new
            m_two = m_new * LOG2E
            s_s[:, cols] = s_s[:, cols] * jnp.exp2(m_old * LOG2E - m_two) + jnp.sum(jnp.exp2(t * LOG2E - m_two[None]), axis=0)

        pipeline(process)

        @pl.when(j == n_tiles - 1)
        def _():
            top = jnp.max(m_s[...], axis=0, keepdims=True)
            total = jnp.sum(s_s[...] * jnp.exp2((m_s[...] - top) * LOG2E), axis=0, keepdims=True)
            lse = top * LOG2E + jnp.log2(total)
            bias_s[0:1, :] = lse - jnp.log2(coef_ref[...])
            bias_s[1:2, :] = lse
            dhn_ref[...] = jnp.zeros_like(dhn_ref)

    @pl.when(phase == 1)
    def _():
        def back(b):
            cols = pl.ds(b * tb, tb)
            dhn_ref[cols, :] += lax.dot_general(dl_ref[:, cols], e_ref[...], TOK_CONTRACT, preferred_element_type=jnp.float32)

        sub = lax.broadcasted_iota(jnp.int32, (8, tb), 0)

        def process(unit, t):
            b, r = unit
            cols = pl.ds(b * tb, tb)
            if r == 0 and b > 0:
                back(b - 1)
            rel = lab_ref[:, cols] - (j * vt + r * ur) - sub
            row = lax.broadcasted_iota(jnp.int32, (ur // 8, 8, tb), 0) * 8
            is_label = row == rel[None]
            prob = jnp.exp2(t * LOG2E - bias_s[0:1, cols][None])
            dl = jnp.where(is_label, prob - coef_ref[:, cols][None], prob)
            pick = pick_s[:, cols]
            for g in range(ur // 8):
                pick = jnp.where(is_label[g], t[g], pick)
            pick_s[:, cols] = pick
            dl_ref[r * ur : (r + 1) * ur, cols] = dl.reshape(ur, tb).astype(jnp.bfloat16)

        pipeline(process)
        back(n_tok // tb - 1)

        @pl.when(j == n_tiles - 1)
        def _():
            picked = jnp.sum(pick_s[...], axis=0, keepdims=True)
            loss_ref[...] = coef_ref[...] * (bias_s[1:2, :] * LN2 - picked)


def head(h_norm_t, table, tok_labels, tok_coef):
    n_tok, vocab = h_norm_t.shape[1], table.shape[0]
    whole = lambda p, j: (0, 0)
    return pl.pallas_call(
        head_kernel,
        grid=(2, vocab // VOCAB_TILE),
        in_specs=[pl.BlockSpec((256, n_tok), whole), pl.BlockSpec((VOCAB_TILE, 256), lambda p, j: (j, 0)), pl.BlockSpec((1, n_tok), whole), pl.BlockSpec((1, n_tok), whole)],
        out_specs=[pl.BlockSpec((VOCAB_TILE, n_tok), lambda p, j: (p * j, 0)), pl.BlockSpec((n_tok, 256), whole), pl.BlockSpec((1, n_tok), whole)],
        out_shape=(jax.ShapeDtypeStruct((vocab, n_tok), jnp.bfloat16), jax.ShapeDtypeStruct((n_tok, 256), jnp.float32), jax.ShapeDtypeStruct((1, n_tok), jnp.float32)),
        scratch_shapes=[pltpu.VMEM((8, n_tok), jnp.float32)] * 3 + [pltpu.VMEM((2, n_tok), jnp.float32)],
        compiler_params=pltpu.CompilerParams(dimension_semantics=("arbitrary", "arbitrary"), vmem_limit_bytes=60 * 1024 * 1024),
        name="head",
    )(h_norm_t, table, tok_labels, tok_coef)


def mlp_backward(saved, d_hidden, gain_mlp, w_gate, w_up, w_down):
    emb_wide, inv_first, a_norm, gate_wide, up_wide, gate_sig, act_rows = saved[:7]
    hid_grad = d_hidden.astype(jnp.bfloat16)
    d_act = lax.dot_general(hid_grad, w_down, ROW_CONTRACT, preferred_element_type=jnp.float32)
    grad_down = lax.dot_general(act_rows, hid_grad, TOK_CONTRACT, preferred_element_type=jnp.float32)
    d_up = (d_act * gate_wide * gate_sig).astype(jnp.bfloat16)
    d_gate = (d_act * up_wide * gate_sig * (1.0 + gate_wide * (1.0 - gate_sig))).astype(jnp.bfloat16)
    grad_gate = lax.dot_general(a_norm, d_gate, TOK_CONTRACT, preferred_element_type=jnp.float32)
    grad_up = lax.dot_general(a_norm, d_up, TOK_CONTRACT, preferred_element_type=jnp.float32)
    d_anorm = lax.dot_general(d_gate, w_gate, ROW_CONTRACT, preferred_element_type=jnp.float32) + lax.dot_general(d_up, w_up, ROW_CONTRACT, preferred_element_type=jnp.float32)
    grad_x = d_hidden + rms_back(emb_wide, inv_first, gain_mlp, d_anorm)
    return grad_x, grad_gate, grad_up, grad_down


def three_parts(wide):
    high = lax.reduce_precision(wide, 8, 7)
    middle = lax.reduce_precision(wide - high, 8, 7)
    return jnp.concatenate([high, middle, wide - high - middle], axis=1).astype(jnp.bfloat16)


def rows_to_tiles(rows):
    return rows.reshape(-1, 8, 8, 256).transpose(0, 2, 1, 3).reshape(-1, 64, 256)


def tiles_to_rows(tiles):
    return tiles.reshape(-1, 8, 8, 256).transpose(0, 2, 1, 3).reshape(-1, 2048)


def solution(mesh):
    def device_step(tok_ids, tok_labels, loss_mask, table_shard, gain_mlp, gain_head, gate_shard, up_shard, down_shard):
        mask_wide = loss_mask.astype(jnp.float32)
        w_shard = jnp.concatenate([rows_to_tiles(gate_shard)[0], rows_to_tiles(up_shard)[0], down_shard], axis=0)
        table_blocks, w_blocks, mask_total = gather_all(table_shard, w_shard, jnp.broadcast_to(jnp.sum(mask_wide), (8, 128)))
        tok_coef = mask_wide / mask_total[0, 0]
        table_full = table_blocks.reshape(-1, 256)
        gate_full = tiles_to_rows(w_blocks[:, 0:64])
        up_full = tiles_to_rows(w_blocks[:, 64:128])
        down_full = w_blocks[:, 128:192].reshape(-1, 256)
        emb_rows = jnp.take(table_full, tok_ids, axis=0)
        saved, h_norm = mlp_forward(emb_rows, gain_mlp, gain_head, gate_full, up_full, down_full)
        d_logits_t, d_hnorm, tok_loss = head(h_norm.T, table_full, tok_labels[None], tok_coef[None])
        d_hidden = rms_back(saved[7], saved[8], gain_head, d_hnorm)
        grad_x, grad_gate, grad_up, grad_down = mlp_backward(saved, d_hidden, gain_mlp, gate_full, up_full, down_full)
        out, loss = scatter_all(d_logits_t, h_norm, three_parts(0.5 * grad_x), tok_ids[None], rows_to_tiles(grad_gate), rows_to_tiles(grad_up), grad_down, jnp.broadcast_to(jnp.sum(tok_loss), (8, 128)))
        g_tab = out[W_CHUNKS:].reshape(E_ROWS, 256)
        return loss[0, 0], g_tab, tiles_to_rows(out[0]), tiles_to_rows(out[1]), out[2]

    row_spec = P("fsdp", None)
    tok_spec = P("fsdp")
    return jax.shard_map(device_step, mesh=mesh, in_specs=(tok_spec, tok_spec, tok_spec, row_spec, P(), P(), row_spec, row_spec, row_spec), out_specs=(P(), row_spec, row_spec, row_spec, row_spec), check_vma=False)
```

```python
import functools

import jax
import jax.numpy as jnp
from jax import lax
from jax.experimental import pallas as pl
from jax.experimental.pallas import tpu as pltpu
from jax.sharding import PartitionSpec as P

NORM_EPS = 1e-6
ROW_CONTRACT = (((1,), (1,)), ((), ()))
TOK_CONTRACT = (((0,), (0,)), ((), ()))
MESH = pl.DeviceIdType.MESH
N_DEV = 32
E_ROWS = 640
W_ROWS = 192
SPLIT = 416
CHUNK = 32
HALF = CHUNK // 2
E_CHUNKS = E_ROWS // CHUNK
N_CHUNKS = (E_ROWS + W_ROWS) // CHUNK
LAG = 2
AHEAD = 3
W_CHUNKS = W_ROWS // CHUNK
PER_W = 64 // CHUNK
Z_PART = 128 // CHUNK
LOG2E = 1.4426950408889634
RANGE = 40.0
LN2 = 0.6931471805599453
VOCAB_TILE = 2048
UNIT = 512
TOK_TILE = 256
PIECES = 6
ORDER = (5, 0, 1, 2, 3, 4)


def dev_index(z, y, x, c):
    return z * 8 + y * 4 + x * 2 + c


def my_coords():
    me = lax.axis_index("fsdp")
    return me // 8, (me // 4) % 2, (me // 2) % 2, me % 2


def z_partners(z):
    return (z + 1 - 2 * (z % 2), (z + 2) % 4, 3 - z)


def greet(z, y, x, c):
    barrier = pltpu.get_barrier_semaphore()
    partners = [dev_index(z, y, x, 1 - c), dev_index(z, y, 1 - x, c), dev_index(z, 1 - y, x, c)]
    partners += [dev_index(zp, y, x, c) for zp in z_partners(z)]
    for dev in partners:
        pl.semaphore_signal(barrier, inc=1, device_id=(dev,), device_id_type=MESH)
    pl.semaphore_wait(barrier, 6)


def gather_kernel(e_ref, g_ref, u_ref, d_ref, mask_ref, eo_ref, go_ref, uo_ref, do_ref, n_ref, m_ref, tiles, send_sem, recv_sem, own_sem):
    z, y, x, c = my_coords()
    me = dev_index(z, y, x, c)
    zs = (z,) + z_partners(z)
    m_ref[...] = jnp.full_like(m_ref, jnp.sum(mask_ref[...].astype(jnp.float32)))
    greet(z, y, x, c)

    own_src = (e_ref.at[pl.ds(0, SPLIT)], e_ref.at[pl.ds(SPLIT, E_ROWS - SPLIT)], g_ref, u_ref, d_ref, m_ref)

    def place(piece, block):
        if piece == 0:
            return eo_ref.at[block, pl.ds(0, SPLIT)]
        if piece == 1:
            return eo_ref.at[block, pl.ds(SPLIT, E_ROWS - SPLIT)]
        return (go_ref, uo_ref, do_ref, tiles)[piece - 2].at[block]

    sent = []
    counts = [0] * PIECES

    def send(piece, block, target, own=False):
        src = own_src[piece] if own else place(piece, block)
        copy = pltpu.make_async_remote_copy(src_ref=src, dst_ref=place(piece, block), send_sem=send_sem.at[piece, counts[piece]], recv_sem=recv_sem.at[piece, block], device_id=(target,), device_id_type=MESH)
        counts[piece] += 1
        copy.start()
        sent.append(copy)

    def arrive(piece, block):
        ref = place(piece, block)
        pltpu.make_async_copy(ref, ref, recv_sem.at[piece, block]).wait()

    to_core = dev_index(z, y, x, 1 - c)
    to_x = dev_index(z, y, 1 - x, c)
    to_y = dev_index(z, 1 - y, x, c)
    hops = ((to_y, to_x), (to_x, to_y), (to_x, to_y), (to_x, to_y), (to_x, to_y), (to_y, to_x))

    def block_at(piece, depth, k, j=0):
        if piece in (0, 5):
            ys, xs = ((y, x), (1 - y, x), ((y, 1 - y)[j], 1 - x))[depth]
        else:
            ys, xs = ((y, x), (y, 1 - x), (1 - y, (x, 1 - x)[j]))[depth]
        return dev_index(zs[k], ys, xs, c)

    for k in (1, 2, 3):
        for piece in ORDER:
            send(piece, me, dev_index(zs[k], y, x, c), own=True)
    for piece in ORDER:
        send(piece, me, hops[piece][0], own=True)
    for piece in ORDER:
        send(piece, me, hops[piece][1], own=True)
    for piece in ORDER:
        send(piece, me, to_core, own=True)
    keep = [pltpu.make_async_copy(own_src[piece], place(piece, me), own_sem.at[piece]) for piece in ORDER]
    for copy in keep:
        copy.start()

    for step in range(6):
        if 1 <= step < 4:
            for piece in ORDER:
                block = block_at(piece, 0, step)
                arrive(piece, block)
                send(piece, block, hops[piece][0])
                send(piece, block, hops[piece][1])
                send(piece, block, to_core)
        if 1 <= step < 5:
            for piece in ORDER:
                block = block_at(piece, 1, step - 1)
                arrive(piece, block)
                send(piece, block, hops[piece][1])
                send(piece, block, to_core)
        if 2 <= step < 6:
            for j in range(2):
                for piece in ORDER:
                    block = block_at(piece, 2, step - 2, j)
                    arrive(piece, block)
                    send(piece, block, to_core)
    for zb in range(4):
        for yb in range(2):
            for xb in range(2):
                for piece in ORDER:
                    arrive(piece, dev_index(zb, yb, xb, 1 - c))
    for copy in sent:
        copy.wait_send()
    for copy in keep:
        copy.wait()

    def total(i, acc):
        return acc + tiles[i]

    n_ref[...] = lax.fori_loop(0, N_DEV, total, jnp.zeros_like(n_ref))


def gather_all(e_shard, gate_shard, up_shard, down_shard, mask_tile):
    vmem = pl.BlockSpec(memory_space=pltpu.VMEM)
    anyspace = pl.BlockSpec(memory_space=pl.ANY)
    shards = (e_shard, gate_shard, up_shard, down_shard)
    return pl.pallas_call(
        gather_kernel,
        out_shape=(*(jax.ShapeDtypeStruct((N_DEV, *a.shape), a.dtype) for a in shards), jax.ShapeDtypeStruct((8, 128), jnp.float32)),
        in_specs=[vmem] * 5,
        out_specs=(*(anyspace for _ in shards), vmem),
        scratch_shapes=[
            pltpu.VMEM((8, 128), jnp.float32),
            pltpu.VMEM((N_DEV, 8, 128), jnp.float32),
            pltpu.SemaphoreType.DMA((PIECES, N_DEV)),
            pltpu.SemaphoreType.DMA((PIECES, N_DEV)),
            pltpu.SemaphoreType.DMA((PIECES,)),
        ],
        compiler_params=pltpu.CompilerParams(collective_id=0, has_side_effects=True),
        name="gather_all",
    )(*shards, mask_tile)


def scatter_kernel(dl_ref, hn_ref, dx_ref, id_ref, gg_ref, gu_ref, gd_ref, l_ref, oe_ref, ow_ref, loss_ref, acc, r0, r1a, r1b, r2, r3, bufs, dl_buf, away_buf, hot, dx_parts, own_sem, load_sem, s0, q0, s1, q1, s2, q2, s3, q3, small_send, small_recv):
    z, y, x, c = my_coords()
    to_core = dev_index(z, y, x, 1 - c)
    to_x = dev_index(z, y, 1 - x, c)
    to_y = dev_index(z, 1 - y, x, c)
    zs = z_partners(z)
    greet(z, y, x, c)

    def remote(src, dst, send_sem, recv_sem, dev):
        return pltpu.make_async_remote_copy(src_ref=src, dst_ref=dst, send_sem=send_sem, recv_sem=recv_sem, device_id=(dev,), device_id_type=MESH)

    def core_away(k, src):
        return remote(src, r0.at[k], s0.at[k], q0.at[k], to_core)

    def load(k):
        slot = k % 2
        return pltpu.make_async_copy(dl_ref.at[:, :, :, :, pl.ds((k - W_CHUNKS) * CHUNK, CHUNK)], dl_buf.at[slot], load_sem.at[slot])

    def table_rows(k):
        slot = k % 2
        load(k).wait()

        @pl.when(k >= W_CHUNKS + 2)
        def _():
            core_away(k - 2, away_buf.at[slot]).wait_send()

        row = lax.broadcasted_iota(jnp.int32, (CHUNK, id_ref.shape[1]), 0)
        hn = hn_ref[...]
        dx = dx_parts[...]
        for mine in range(2):
            core = c if mine else 1 - c

            def part(zp, carry, mine=mine, core=core):
                for i in range(4 * Z_PART):
                    dev = dev_index(Z_PART * zp + i // 4, (i // 2) % 2, i % 2, core)
                    here = row == id_ref[...] - (dev * E_ROWS + (k - W_CHUNKS) * CHUNK)
                    hot[i * CHUNK : (i + 1) * CHUNK] = jnp.where(here, 1.0, 0.0).astype(jnp.bfloat16)
                head = jnp.dot(dl_buf[slot, pl.ds(Z_PART * zp, Z_PART), :, :, core].reshape(512, -1), hn, preferred_element_type=jnp.float32)
                rows = jnp.dot(hot[...], dx, preferred_element_type=jnp.float32)
                rows = rows[:, 0:256] + (rows[:, 256:512] + rows[:, 512:768])
                total = (head + 2.0 * rows).reshape(Z_PART, 2, 2, CHUNK, 256)
                if mine:
                    acc[k, pl.ds(Z_PART * zp, Z_PART)] = total
                else:
                    away_buf[slot, pl.ds(Z_PART * zp, Z_PART)] = total
                return carry

            lax.fori_loop(0, 4 // Z_PART, part, 0)
            if not mine:
                core_away(k, away_buf.at[slot]).start()

        @pl.when(k + 2 < N_CHUNKS)
        def _():
            load(k + 2).start()

    def plane_first(k):
        return (
            remote(acc.at[k, :, :, 1 - x, pl.ds(0, HALF)], r1a.at[k], s1.at[0, k], q1.at[0, k], to_x),
            remote(acc.at[k, :, 1 - y, :, pl.ds(HALF, HALF)], r1b.at[k], s1.at[1, k], q1.at[1, k], to_y),
        )

    def plane_second(k):
        return (
            remote(r1a.at[k, :, 1 - y], r2.at[k, :, pl.ds(0, HALF)], s2.at[0, k], q2.at[0, k], to_y),
            remote(r1b.at[k, :, 1 - x], r2.at[k, :, pl.ds(HALF, HALF)], s2.at[1, k], q2.at[1, k], to_x),
        )

    def along_z(k):
        return tuple(remote(r2.at[k, zs[i]], r3.at[k, i], s3.at[i, k], q3.at[i, k], dev_index(zs[i], y, x, c)) for i in range(3))

    def small(src, slot, dev):
        return remote(src, bufs.at[slot], small_send.at[slot], small_recv.at[slot], dev)

    small_steps = (
        (small(l_ref, 0, to_core),),
        (small(bufs.at[6], 1, to_x),),
        (small(bufs.at[7], 2, to_y),),
        tuple(small(bufs.at[8], 3 + i, dev_index(zs[i], y, x, c)) for i in range(3)),
    )
    small_steps[0][0].start()
    w_refs = (gg_ref, gu_ref, gd_ref)
    for k in range(W_CHUNKS):
        rows = pl.ds(k % PER_W * CHUNK, CHUNK)
        core_away(k, w_refs[k // PER_W].at[:, :, :, 1 - c, rows]).start()
        pltpu.make_async_copy(w_refs[k // PER_W].at[:, :, :, c, rows], acc.at[k], own_sem.at[k]).start()
    for k in range(W_CHUNKS, W_CHUNKS + 2):
        load(k).start()

    def cut(i, carry):
        rows = pl.ds(pl.multiple_of(i * 128, 128), 128)
        wide = 0.5 * dx_ref[rows, :]
        for j in range(3):
            part = wide.astype(jnp.bfloat16)
            dx_parts[rows, j * 256 : (j + 1) * 256] = part
            wide = wide - part.astype(jnp.float32)
        return carry

    lax.fori_loop(0, dx_ref.shape[0] // 128, cut, 0)

    def step_body(s, carry):
        @pl.when(s < W_CHUNKS)
        def _():
            pltpu.make_async_copy(acc.at[s], acc.at[s], own_sem.at[s]).wait()

        @pl.when(s < N_CHUNKS)
        def _():
            core_away(s, r0.at[s]).wait_recv()

            def add(i, inner):
                acc[s, i // 4, (i // 2) % 2, i % 2] += r0[s, i // 4, (i // 2) % 2, i % 2]
                return inner

            lax.fori_loop(0, 16, add, 0)
            for copy in plane_first(s):
                copy.start()

        @pl.when((s >= LAG) & (s < N_CHUNKS + LAG))
        def _():
            k = s - LAG
            for copy in plane_first(k):
                copy.wait_recv()

            def add(i, inner):
                r1a[k, i // 2, i % 2] += acc[k, i // 2, i % 2, x, pl.ds(0, HALF)]
                r1b[k, i // 2, i % 2] += acc[k, i // 2, y, i % 2, pl.ds(HALF, HALF)]
                return inner

            lax.fori_loop(0, 8, add, 0)
            for copy in plane_second(k):
                copy.start()

        @pl.when((s >= 2 * LAG) & (s < N_CHUNKS + 2 * LAG))
        def _():
            k = s - 2 * LAG
            for copy in plane_second(k):
                copy.wait_recv()

            def add(i, inner):
                r2[k, i, pl.ds(0, HALF)] += r1a[k, i, y]
                r2[k, i, pl.ds(HALF, HALF)] += r1b[k, i, x]
                return inner

            lax.fori_loop(0, 4, add, 0)
            for copy in along_z(k):
                copy.start()

        @pl.when(s >= 3 * LAG)
        def _():
            k = s - 3 * LAG
            for copy in along_z(k):
                copy.wait_recv()
            total = (r2[k, z] + r3[k, 0]) + (r3[k, 1] + r3[k, 2])
            @pl.when(k < W_CHUNKS)
            def _():
                ow_ref[k] = total

            @pl.when(k >= W_CHUNKS)
            def _():
                oe_ref[pl.ds(pl.multiple_of((k - W_CHUNKS) * CHUNK, CHUNK), CHUNK)] = total

        @pl.when((s + AHEAD >= W_CHUNKS) & (s + AHEAD < N_CHUNKS))
        def _():
            table_rows(s + AHEAD)

        for i in range(3):

            @pl.when(s == 1 + 3 * i)
            def _():
                small_steps[i][0].wait()
                bufs[6 + i] = (l_ref[...] if i == 0 else bufs[5 + i]) + bufs[i]
                for copy in small_steps[i + 1]:
                    copy.start()

        return carry

    lax.fori_loop(0, N_CHUNKS + 3 * LAG, step_body, 0)

    for copy in small_steps[3]:
        copy.wait()
    loss_ref[...] = ((bufs[8] + bufs[3]) + (bufs[4] + bufs[5]))[0:1, 0:1]

    for k in (*range(W_CHUNKS), N_CHUNKS - 2, N_CHUNKS - 1):
        core_away(k, r0.at[k]).wait_send()

    def finish(k, carry):
        for copy in plane_first(k) + plane_second(k) + along_z(k):
            copy.wait_send()
        return carry

    lax.fori_loop(0, N_CHUNKS, finish, 0)


def scatter_all(d_logits_t, h_norm, grad_x, tok_ids, grad_gate, grad_up, grad_down, loss_tile):
    vmem = pl.BlockSpec(memory_space=pltpu.VMEM)
    anyspace = pl.BlockSpec(memory_space=pl.ANY)
    dma = pltpu.SemaphoreType.DMA
    n_tok = h_norm.shape[0]
    mesh_rows = (4, 2, 2, 2)
    return pl.pallas_call(
        scatter_kernel,
        out_shape=tuple(jax.ShapeDtypeStruct(shape, jnp.float32) for shape in ((E_ROWS, 256), (W_CHUNKS, CHUNK, 256), (1, 1))),
        in_specs=[anyspace, vmem, vmem, vmem, anyspace, anyspace, anyspace, vmem],
        out_specs=(vmem,) * 3,
        scratch_shapes=[
            pltpu.VMEM((N_CHUNKS, 4, 2, 2, CHUNK, 256), jnp.float32),
            pltpu.VMEM((N_CHUNKS, 4, 2, 2, CHUNK, 256), jnp.float32),
            pltpu.VMEM((N_CHUNKS, 4, 2, HALF, 256), jnp.float32),
            pltpu.VMEM((N_CHUNKS, 4, 2, HALF, 256), jnp.float32),
            pltpu.VMEM((N_CHUNKS, 4, CHUNK, 256), jnp.float32),
            pltpu.VMEM((N_CHUNKS, 3, CHUNK, 256), jnp.float32),
            pltpu.VMEM((9, 8, 128), jnp.float32),
            pltpu.VMEM((2, *mesh_rows, CHUNK, n_tok), jnp.bfloat16),
            pltpu.VMEM((2, 4, 2, 2, CHUNK, 256), jnp.float32),
            pltpu.VMEM((512, n_tok), jnp.bfloat16),
            pltpu.VMEM((n_tok, 768), jnp.bfloat16),
            dma((W_CHUNKS,)),
            dma((2,)),
            dma((N_CHUNKS,)),
            dma((N_CHUNKS,)),
            dma((2, N_CHUNKS)),
            dma((2, N_CHUNKS)),
            dma((2, N_CHUNKS)),
            dma((2, N_CHUNKS)),
            dma((3, N_CHUNKS)),
            dma((3, N_CHUNKS)),
            dma((6,)),
            dma((6,)),
        ],
        compiler_params=pltpu.CompilerParams(collective_id=1, has_side_effects=True, vmem_limit_bytes=63 * 1024 * 1024),
        name="scatter_all",
    )(d_logits_t.reshape(*mesh_rows, E_ROWS, n_tok), h_norm, grad_x, tok_ids, *(g.reshape(*mesh_rows, 64, 256) for g in (grad_gate, grad_up, grad_down)), loss_tile)


def rms_scale(rows_wide, norm_gain):
    inv_rms = lax.rsqrt(jnp.mean(rows_wide * rows_wide, axis=-1, keepdims=True) + NORM_EPS)
    return (rows_wide * inv_rms * norm_gain).astype(jnp.bfloat16), inv_rms


def rms_back(rows_wide, inv_rms, norm_gain, grad_out):
    scaled_grad = grad_out * norm_gain
    return inv_rms * (scaled_grad - rows_wide * (inv_rms * inv_rms) * jnp.mean(scaled_grad * rows_wide, axis=-1, keepdims=True))


def mlp_forward(emb_rows, gain_mlp, gain_head, w_gate, w_up, w_down):
    emb_wide = emb_rows.astype(jnp.float32)
    a_norm, inv_first = rms_scale(emb_wide, gain_mlp)
    gate_wide = jnp.dot(a_norm, w_gate, preferred_element_type=jnp.float32).astype(jnp.bfloat16).astype(jnp.float32)
    up_wide = jnp.dot(a_norm, w_up, preferred_element_type=jnp.float32).astype(jnp.bfloat16).astype(jnp.float32)
    gate_sig = jax.nn.sigmoid(gate_wide)
    act_rows = (gate_wide * gate_sig * up_wide).astype(jnp.bfloat16)
    hid_wide = (emb_wide + jnp.dot(act_rows, w_down, preferred_element_type=jnp.float32)).astype(jnp.bfloat16).astype(jnp.float32)
    h_norm, inv_second = rms_scale(hid_wide, gain_head)
    return (emb_wide, inv_first, a_norm, gate_wide, up_wide, gate_sig, act_rows, hid_wide, inv_second), h_norm


def head_kernel(hn_ref, e_ref, lab_ref, mask_ref, n_ref, dl_ref, dhn_ref, loss_ref, ht_ref, m_s, s_s, pick_s, bias_s, coef_ref, redo):
    phase, j = pl.program_id(0), pl.program_id(1)
    n_tok = ht_ref.shape[1]
    n_tiles = pl.num_programs(1)
    vt, ur, tb = VOCAB_TILE, UNIT, TOK_TILE
    units = [(b, r) for b in range(n_tok // tb) for r in range(vt // ur)]

    def scaled(unit):
        b, r = unit
        return jnp.dot(e_ref[r * ur : (r + 1) * ur], ht_ref[:, b * tb : (b + 1) * tb], preferred_element_type=jnp.float32)

    def pipeline(process):
        ahead = scaled(units[0])
        for i, unit in enumerate(units):
            now = ahead
            if i + 1 < len(units):
                ahead = scaled(units[i + 1])
            process(unit, now.reshape(ur // 8, 8, tb))

    @pl.when(phase == 0)
    def _():
        @pl.when(j == 0)
        def _():
            ht_ref[...] = hn_ref[...].T
            coef_ref[...] = mask_ref[...].astype(jnp.float32) / n_ref[0:1, 0:1]
            m_s[...] = jnp.full_like(m_s, -jnp.inf)
            s_s[...] = jnp.zeros_like(s_s)
            pick_s[...] = jnp.zeros_like(pick_s)
            redo[0] = 1

        @pl.when(j > 0)
        def _():
            sums, tops = {}, {}

            def process(unit, t):
                b = unit[0]
                point = m_s[:, b * tb : (b + 1) * tb] * LOG2E
                part = jnp.exp2(t[0] * LOG2E - point)
                top = t[0]
                for g in range(1, ur // 8):
                    part += jnp.exp2(t[g] * LOG2E - point)
                    top = jnp.maximum(top, t[g])
                sums[b] = sums[b] + part if b in sums else part
                tops[b] = jnp.maximum(tops[b], top) if b in tops else top

            pipeline(process)
            over = jnp.max(jnp.concatenate([tops[b] - m_s[:, b * tb : (b + 1) * tb] for b in tops], axis=1))
            fits = over <= RANGE
            redo[0] = jnp.where(fits, 0, 1)
            for b in sums:
                s_s[:, b * tb : (b + 1) * tb] += jnp.where(fits, sums[b], 0.0)

        @pl.when(redo[0] == 1)
        def _():
            def process(unit, t):
                cols = pl.ds(unit[0] * tb, tb)
                m_old = m_s[:, cols]
                m_new = jnp.maximum(m_old, jnp.max(t, axis=0))
                m_s[:, cols] = m_new
                m_two = m_new * LOG2E
                s_s[:, cols] = s_s[:, cols] * jnp.exp2(m_old * LOG2E - m_two) + jnp.sum(jnp.exp2(t * LOG2E - m_two[None]), axis=0)

            pipeline(process)

        @pl.when(j == n_tiles - 1)
        def _():
            top = jnp.max(m_s[...], axis=0, keepdims=True)
            total = jnp.sum(s_s[...] * jnp.exp2((m_s[...] - top) * LOG2E), axis=0, keepdims=True)
            lse = top * LOG2E + jnp.log2(total)
            bias_s[0:1, :] = lse - jnp.log2(coef_ref[...])
            bias_s[1:2, :] = lse
            dhn_ref[...] = jnp.zeros_like(dhn_ref)

    @pl.when(phase == 1)
    def _():
        def back(b):
            cols = pl.ds(b * tb, tb)
            dhn_ref[cols, :] += lax.dot_general(dl_ref[:, cols], e_ref[...], TOK_CONTRACT, preferred_element_type=jnp.float32)

        sub = lax.broadcasted_iota(jnp.int32, (8, tb), 0)

        def process(unit, t):
            b, r = unit
            cols = pl.ds(b * tb, tb)
            if r == 0 and b > 0:
                back(b - 1)
            rel = lab_ref[:, cols] - (j * vt + r * ur) - sub
            row = lax.broadcasted_iota(jnp.int32, (ur // 8, 8, tb), 0) * 8
            is_label = row == rel[None]
            prob = jnp.exp2(t * LOG2E - bias_s[0:1, cols][None])
            dl = jnp.where(is_label, prob - coef_ref[:, cols][None], prob)
            pick = pick_s[:, cols]
            for g in range(ur // 8):
                pick = jnp.where(is_label[g], t[g], pick)
            pick_s[:, cols] = pick
            dl_ref[r * ur : (r + 1) * ur, cols] = dl.reshape(ur, tb).astype(jnp.bfloat16)

        pipeline(process)
        back(n_tok // tb - 1)

        @pl.when(j == n_tiles - 1)
        def _():
            picked = jnp.sum(pick_s[...], axis=0, keepdims=True)
            loss_ref[...] = jnp.full_like(loss_ref, jnp.sum(coef_ref[...] * (bias_s[1:2, :] * LN2 - picked)))


def head(h_norm, table, tok_labels, loss_mask, mask_total):
    n_tok, vocab = h_norm.shape[0], table.shape[0]

    def whole(*shape):
        return pl.BlockSpec(shape, lambda p, j: (0, 0))

    return pl.pallas_call(
        head_kernel,
        grid=(2, vocab // VOCAB_TILE),
        in_specs=[whole(n_tok, 256), pl.BlockSpec((VOCAB_TILE, 256), lambda p, j: (j, 0)), whole(1, n_tok), whole(1, n_tok), whole(8, 128)],
        out_specs=[pl.BlockSpec((VOCAB_TILE, n_tok), lambda p, j: (p * j, 0)), whole(n_tok, 256), whole(8, 128)],
        out_shape=(jax.ShapeDtypeStruct((vocab, n_tok), jnp.bfloat16), jax.ShapeDtypeStruct((n_tok, 256), jnp.float32), jax.ShapeDtypeStruct((8, 128), jnp.float32)),
        scratch_shapes=[pltpu.VMEM((256, n_tok), jnp.bfloat16)] + [pltpu.VMEM((8, n_tok), jnp.float32)] * 3 + [pltpu.VMEM((2, n_tok), jnp.float32), pltpu.VMEM((1, n_tok), jnp.float32), pltpu.SMEM((1,), jnp.int32)],
        compiler_params=pltpu.CompilerParams(dimension_semantics=("arbitrary", "arbitrary"), vmem_limit_bytes=60 * 1024 * 1024),
        name="head",
    )(h_norm, table, tok_labels, loss_mask, mask_total)


def mlp_backward(saved, d_hidden, gain_mlp, w_gate, w_up, w_down):
    emb_wide, inv_first, a_norm, gate_wide, up_wide, gate_sig, act_rows = saved[:7]
    hid_grad = d_hidden.astype(jnp.bfloat16)
    d_act = lax.dot_general(hid_grad, w_down, ROW_CONTRACT, preferred_element_type=jnp.float32)
    grad_down = lax.dot_general(act_rows, hid_grad, TOK_CONTRACT, preferred_element_type=jnp.float32)
    d_up = (d_act * gate_wide * gate_sig).astype(jnp.bfloat16)
    d_gate = (d_act * up_wide * gate_sig * (1.0 + gate_wide * (1.0 - gate_sig))).astype(jnp.bfloat16)
    grad_gate = lax.dot_general(a_norm, d_gate, TOK_CONTRACT, preferred_element_type=jnp.float32)
    grad_up = lax.dot_general(a_norm, d_up, TOK_CONTRACT, preferred_element_type=jnp.float32)
    d_anorm = lax.dot_general(d_gate, w_gate, ROW_CONTRACT, preferred_element_type=jnp.float32) + lax.dot_general(d_up, w_up, ROW_CONTRACT, preferred_element_type=jnp.float32)
    grad_x = d_hidden + rms_back(emb_wide, inv_first, gain_mlp, d_anorm)
    return grad_x, grad_gate, grad_up, grad_down


def rows_to_tiles(rows):
    return rows.reshape(-1, 8, 8, 256).transpose(0, 2, 1, 3).reshape(-1, 64, 256)


def tiles_to_rows(tiles):
    return tiles.reshape(8, 8, 256).transpose(1, 0, 2).reshape(8, 2048)


def solution(mesh):
    def device_step(tok_ids, tok_labels, loss_mask, table_shard, gain_mlp, gain_head, gate_shard, up_shard, down_shard):
        table_blocks, gate_blocks, up_blocks, down_blocks, mask_total = gather_all(table_shard, gate_shard, up_shard, down_shard, loss_mask.reshape(8, 128))
        table_full = table_blocks.reshape(-1, 256)
        gate_full = gate_blocks.reshape(-1, 2048)
        up_full = up_blocks.reshape(-1, 2048)
        down_full = down_blocks.reshape(-1, 256)
        emb_rows = jnp.take(table_full, tok_ids, axis=0)
        saved, h_norm = mlp_forward(emb_rows, gain_mlp, gain_head, gate_full, up_full, down_full)
        d_logits_t, d_hnorm, loss_tile = head(h_norm, table_full, tok_labels[None], loss_mask[None], mask_total)
        d_hidden = rms_back(saved[7], saved[8], gain_head, d_hnorm)
        grad_x, grad_gate, grad_up, grad_down = mlp_backward(saved, d_hidden, gain_mlp, gate_full, up_full, down_full)
        d_table, d_weights, loss = scatter_all(d_logits_t, h_norm, grad_x, tok_ids[None], rows_to_tiles(grad_gate), rows_to_tiles(grad_up), grad_down, loss_tile)
        d_gate, d_up, d_down = d_weights.reshape(3, 64, 256)
        return loss.reshape(()), d_table, tiles_to_rows(d_gate), tiles_to_rows(d_up), d_down

    row_spec = P("fsdp", None)
    tok_spec = P("fsdp")
    return jax.shard_map(device_step, mesh=mesh, in_specs=(tok_spec, tok_spec, tok_spec, row_spec, P(), P(), row_spec, row_spec, row_spec), out_specs=(P(), row_spec, row_spec, row_spec, row_spec), check_vma=False)
```

```python
import functools

import jax
import jax.numpy as jnp
from jax import lax
from jax.experimental import pallas as pl
from jax.experimental.pallas import tpu as pltpu
from jax.sharding import PartitionSpec as P

NORM_EPS = 1e-6
ROW_CONTRACT = (((1,), (1,)), ((), ()))
TOK_CONTRACT = (((0,), (0,)), ((), ()))
MESH = pl.DeviceIdType.MESH
N_DEV = 32
E_ROWS = 640
W_ROWS = 192
SPLIT = 416
CHUNK = 32
HALF = CHUNK // 2
E_CHUNKS = E_ROWS // CHUNK
N_CHUNKS = (E_ROWS + W_ROWS) // CHUNK
LAG = 2
AHEAD = 3
W_CHUNKS = W_ROWS // CHUNK
PER_W = 64 // CHUNK
Z_PART = 128 // CHUNK
LOG2E = 1.4426950408889634
RANGE = 40.0
LN2 = 0.6931471805599453
VOCAB_TILE = 2048
FF_TILE = 512
VMEM_LIMIT = 66060288
UNIT = 512
TOK_TILE = 256
PIECES = 6
ORDER = (5, 0, 1, 2, 3, 4)


def dev_index(z, y, x, c):
    return z * 8 + y * 4 + x * 2 + c


def my_coords():
    me = lax.axis_index("fsdp")
    return me // 8, (me // 4) % 2, (me // 2) % 2, me % 2


def z_partners(z):
    return (z + 1 - 2 * (z % 2), (z + 2) % 4, 3 - z)


def greet(z, y, x, c):
    barrier = pltpu.get_barrier_semaphore()
    partners = [dev_index(z, y, x, 1 - c), dev_index(z, y, 1 - x, c), dev_index(z, 1 - y, x, c)]
    partners += [dev_index(zp, y, x, c) for zp in z_partners(z)]
    for dev in partners:
        pl.semaphore_signal(barrier, inc=1, device_id=(dev,), device_id_type=MESH)
    pl.semaphore_wait(barrier, 6)


def gather_kernel(e_ref, g_ref, u_ref, d_ref, mask_ref, eo_ref, go_ref, uo_ref, do_ref, n_ref, m_ref, tiles, send_sem, recv_sem, own_sem):
    z, y, x, c = my_coords()
    me = dev_index(z, y, x, c)
    zs = (z,) + z_partners(z)
    m_ref[...] = jnp.full_like(m_ref, jnp.sum(mask_ref[...].astype(jnp.float32)))
    greet(z, y, x, c)

    own_src = (e_ref.at[pl.ds(0, SPLIT)], e_ref.at[pl.ds(SPLIT, E_ROWS - SPLIT)], g_ref, u_ref, d_ref, m_ref)

    def place(piece, block):
        if piece == 0:
            return eo_ref.at[block, pl.ds(0, SPLIT)]
        if piece == 1:
            return eo_ref.at[block, pl.ds(SPLIT, E_ROWS - SPLIT)]
        return (go_ref, uo_ref, do_ref, tiles)[piece - 2].at[block]

    sent = []
    counts = [0] * PIECES

    def send(piece, block, target, own=False):
        src = own_src[piece] if own else place(piece, block)
        copy = pltpu.make_async_remote_copy(src_ref=src, dst_ref=place(piece, block), send_sem=send_sem.at[piece, counts[piece]], recv_sem=recv_sem.at[piece, block], device_id=(target,), device_id_type=MESH)
        counts[piece] += 1
        copy.start()
        sent.append(copy)

    def arrive(piece, block):
        ref = place(piece, block)
        pltpu.make_async_copy(ref, ref, recv_sem.at[piece, block]).wait()

    to_core = dev_index(z, y, x, 1 - c)
    to_x = dev_index(z, y, 1 - x, c)
    to_y = dev_index(z, 1 - y, x, c)
    hops = ((to_y, to_x), (to_x, to_y), (to_x, to_y), (to_x, to_y), (to_x, to_y), (to_y, to_x))

    def block_at(piece, depth, k, j=0):
        if piece in (0, 5):
            ys, xs = ((y, x), (1 - y, x), ((y, 1 - y)[j], 1 - x))[depth]
        else:
            ys, xs = ((y, x), (y, 1 - x), (1 - y, (x, 1 - x)[j]))[depth]
        return dev_index(zs[k], ys, xs, c)

    for k in (1, 2, 3):
        for piece in ORDER:
            send(piece, me, dev_index(zs[k], y, x, c), own=True)
    for piece in ORDER:
        send(piece, me, hops[piece][0], own=True)
    for piece in ORDER:
        send(piece, me, hops[piece][1], own=True)
    for piece in ORDER:
        send(piece, me, to_core, own=True)
    keep = [pltpu.make_async_copy(own_src[piece], place(piece, me), own_sem.at[piece]) for piece in ORDER]
    for copy in keep:
        copy.start()

    for step in range(6):
        if 1 <= step < 4:
            for piece in ORDER:
                block = block_at(piece, 0, step)
                arrive(piece, block)
                send(piece, block, hops[piece][0])
                send(piece, block, hops[piece][1])
                send(piece, block, to_core)
        if 1 <= step < 5:
            for piece in ORDER:
                block = block_at(piece, 1, step - 1)
                arrive(piece, block)
                send(piece, block, hops[piece][1])
                send(piece, block, to_core)
        if 2 <= step < 6:
            for j in range(2):
                for piece in ORDER:
                    block = block_at(piece, 2, step - 2, j)
                    arrive(piece, block)
                    send(piece, block, to_core)
    for zb in range(4):
        for yb in range(2):
            for xb in range(2):
                for piece in ORDER:
                    arrive(piece, dev_index(zb, yb, xb, 1 - c))
    for copy in sent:
        copy.wait_send()
    for copy in keep:
        copy.wait()

    def total(i, acc):
        return acc + tiles[i]

    n_ref[...] = lax.fori_loop(0, N_DEV, total, jnp.zeros_like(n_ref))


def gather_all(e_shard, gate_shard, up_shard, down_shard, mask_tile):
    vmem = pl.BlockSpec(memory_space=pltpu.VMEM)
    anyspace = pl.BlockSpec(memory_space=pl.ANY)
    shards = (e_shard, gate_shard, up_shard, down_shard)
    return pl.pallas_call(
        gather_kernel,
        out_shape=(*(jax.ShapeDtypeStruct((N_DEV, *a.shape), a.dtype) for a in shards), jax.ShapeDtypeStruct((8, 128), jnp.float32)),
        in_specs=[vmem] * 5,
        out_specs=(*(anyspace for _ in shards), vmem),
        scratch_shapes=[
            pltpu.VMEM((8, 128), jnp.float32),
            pltpu.VMEM((N_DEV, 8, 128), jnp.float32),
            pltpu.SemaphoreType.DMA((PIECES, N_DEV)),
            pltpu.SemaphoreType.DMA((PIECES, N_DEV)),
            pltpu.SemaphoreType.DMA((PIECES,)),
        ],
        compiler_params=pltpu.CompilerParams(collective_id=0, has_side_effects=True),
        name="gather_all",
    )(*shards, mask_tile)


def scatter_kernel(dl_ref, hn_ref, dx_ref, id_ref, gg_ref, gu_ref, gd_ref, l_ref, oe_ref, ow_ref, loss_ref, acc, r0, r1a, r1b, r2, r3, bufs, dl_buf, away_buf, hot, dx_parts, own_sem, load_sem, s0, q0, s1, q1, s2, q2, s3, q3, small_send, small_recv):
    z, y, x, c = my_coords()
    to_core = dev_index(z, y, x, 1 - c)
    to_x = dev_index(z, y, 1 - x, c)
    to_y = dev_index(z, 1 - y, x, c)
    zs = z_partners(z)
    greet(z, y, x, c)

    def remote(src, dst, send_sem, recv_sem, dev):
        return pltpu.make_async_remote_copy(src_ref=src, dst_ref=dst, send_sem=send_sem, recv_sem=recv_sem, device_id=(dev,), device_id_type=MESH)

    def core_away(k, src):
        return remote(src, r0.at[k], s0.at[k], q0.at[k], to_core)

    def load(k):
        slot = k % 2
        return pltpu.make_async_copy(dl_ref.at[:, :, :, :, pl.ds((k - W_CHUNKS) * CHUNK, CHUNK)], dl_buf.at[slot], load_sem.at[slot])

    def table_rows(k):
        slot = k % 2
        load(k).wait()

        @pl.when(k >= W_CHUNKS + 2)
        def _():
            core_away(k - 2, away_buf.at[slot]).wait_send()

        row = lax.broadcasted_iota(jnp.int32, (CHUNK, id_ref.shape[1]), 0)
        hn = hn_ref[...]
        dx = dx_parts[...]
        for mine in range(2):
            core = c if mine else 1 - c

            def part(zp, carry, mine=mine, core=core):
                for i in range(4 * Z_PART):
                    dev = dev_index(Z_PART * zp + i // 4, (i // 2) % 2, i % 2, core)
                    here = row == id_ref[...] - (dev * E_ROWS + (k - W_CHUNKS) * CHUNK)
                    hot[i * CHUNK : (i + 1) * CHUNK] = jnp.where(here, 1.0, 0.0).astype(jnp.bfloat16)
                head = jnp.dot(dl_buf[slot, pl.ds(Z_PART * zp, Z_PART), :, :, core].reshape(512, -1), hn, preferred_element_type=jnp.float32)
                rows = jnp.dot(hot[...], dx, preferred_element_type=jnp.float32)
                rows = rows[:, 0:256] + (rows[:, 256:512] + rows[:, 512:768])
                total = (head + 2.0 * rows).reshape(Z_PART, 2, 2, CHUNK, 256)
                if mine:
                    acc[k, pl.ds(Z_PART * zp, Z_PART)] = total
                else:
                    away_buf[slot, pl.ds(Z_PART * zp, Z_PART)] = total
                return carry

            lax.fori_loop(0, 4 // Z_PART, part, 0)
            if not mine:
                core_away(k, away_buf.at[slot]).start()

        @pl.when(k + 2 < N_CHUNKS)
        def _():
            load(k + 2).start()

    def plane_first(k):
        return (
            remote(acc.at[k, :, :, 1 - x, pl.ds(0, HALF)], r1a.at[k], s1.at[0, k], q1.at[0, k], to_x),
            remote(acc.at[k, :, 1 - y, :, pl.ds(HALF, HALF)], r1b.at[k], s1.at[1, k], q1.at[1, k], to_y),
        )

    def plane_second(k):
        return (
            remote(r1a.at[k, :, 1 - y], r2.at[k, :, pl.ds(0, HALF)], s2.at[0, k], q2.at[0, k], to_y),
            remote(r1b.at[k, :, 1 - x], r2.at[k, :, pl.ds(HALF, HALF)], s2.at[1, k], q2.at[1, k], to_x),
        )

    def along_z(k):
        return tuple(remote(r2.at[k, zs[i]], r3.at[k, i], s3.at[i, k], q3.at[i, k], dev_index(zs[i], y, x, c)) for i in range(3))

    def small(src, slot, dev):
        return remote(src, bufs.at[slot], small_send.at[slot], small_recv.at[slot], dev)

    small_steps = (
        (small(l_ref, 0, to_core),),
        (small(bufs.at[6], 1, to_x),),
        (small(bufs.at[7], 2, to_y),),
        tuple(small(bufs.at[8], 3 + i, dev_index(zs[i], y, x, c)) for i in range(3)),
    )
    small_steps[0][0].start()
    w_refs = (gg_ref, gu_ref, gd_ref)
    for k in range(W_CHUNKS):
        rows = pl.ds(k % PER_W * CHUNK, CHUNK)
        core_away(k, w_refs[k // PER_W].at[:, :, :, 1 - c, rows]).start()
        pltpu.make_async_copy(w_refs[k // PER_W].at[:, :, :, c, rows], acc.at[k], own_sem.at[k]).start()
    for k in range(W_CHUNKS, W_CHUNKS + 2):
        load(k).start()

    def cut(i, carry):
        rows = pl.ds(pl.multiple_of(i * 128, 128), 128)
        wide = 0.5 * dx_ref[rows, :]
        for j in range(3):
            part = wide.astype(jnp.bfloat16)
            dx_parts[rows, j * 256 : (j + 1) * 256] = part
            wide = wide - part.astype(jnp.float32)
        return carry

    lax.fori_loop(0, dx_ref.shape[0] // 128, cut, 0)

    def step_body(s, carry):
        @pl.when(s < W_CHUNKS)
        def _():
            pltpu.make_async_copy(acc.at[s], acc.at[s], own_sem.at[s]).wait()

        @pl.when(s < N_CHUNKS)
        def _():
            core_away(s, r0.at[s]).wait_recv()

            def add(i, inner):
                acc[s, i // 4, (i // 2) % 2, i % 2] += r0[s, i // 4, (i // 2) % 2, i % 2]
                return inner

            lax.fori_loop(0, 16, add, 0)
            for copy in plane_first(s):
                copy.start()

        @pl.when((s >= LAG) & (s < N_CHUNKS + LAG))
        def _():
            k = s - LAG
            for copy in plane_first(k):
                copy.wait_recv()

            def add(i, inner):
                r1a[k, i // 2, i % 2] += acc[k, i // 2, i % 2, x, pl.ds(0, HALF)]
                r1b[k, i // 2, i % 2] += acc[k, i // 2, y, i % 2, pl.ds(HALF, HALF)]
                return inner

            lax.fori_loop(0, 8, add, 0)
            for copy in plane_second(k):
                copy.start()

        @pl.when((s >= 2 * LAG) & (s < N_CHUNKS + 2 * LAG))
        def _():
            k = s - 2 * LAG
            for copy in plane_second(k):
                copy.wait_recv()

            def add(i, inner):
                r2[k, i, pl.ds(0, HALF)] += r1a[k, i, y]
                r2[k, i, pl.ds(HALF, HALF)] += r1b[k, i, x]
                return inner

            lax.fori_loop(0, 4, add, 0)
            for copy in along_z(k):
                copy.start()

        @pl.when(s >= 3 * LAG)
        def _():
            k = s - 3 * LAG
            for copy in along_z(k):
                copy.wait_recv()
            total = (r2[k, z] + r3[k, 0]) + (r3[k, 1] + r3[k, 2])
            @pl.when(k < W_CHUNKS)
            def _():
                ow_ref[k] = total

            @pl.when(k >= W_CHUNKS)
            def _():
                oe_ref[pl.ds(pl.multiple_of((k - W_CHUNKS) * CHUNK, CHUNK), CHUNK)] = total

        @pl.when((s + AHEAD >= W_CHUNKS) & (s + AHEAD < N_CHUNKS))
        def _():
            table_rows(s + AHEAD)

        for i in range(3):

            @pl.when(s == 1 + 3 * i)
            def _():
                small_steps[i][0].wait()
                bufs[6 + i] = (l_ref[...] if i == 0 else bufs[5 + i]) + bufs[i]
                for copy in small_steps[i + 1]:
                    copy.start()

        return carry

    lax.fori_loop(0, N_CHUNKS + 3 * LAG, step_body, 0)

    for copy in small_steps[3]:
        copy.wait()
    loss_ref[...] = ((bufs[8] + bufs[3]) + (bufs[4] + bufs[5]))[0:1, 0:1]

    for k in (*range(W_CHUNKS), N_CHUNKS - 2, N_CHUNKS - 1):
        core_away(k, r0.at[k]).wait_send()

    def finish(k, carry):
        for copy in plane_first(k) + plane_second(k) + along_z(k):
            copy.wait_send()
        return carry

    lax.fori_loop(0, N_CHUNKS, finish, 0)


def scatter_all(d_logits_t, h_norm, grad_x, tok_ids, grad_gate, grad_up, grad_down, loss_tile):
    vmem = pl.BlockSpec(memory_space=pltpu.VMEM)
    anyspace = pl.BlockSpec(memory_space=pl.ANY)
    dma = pltpu.SemaphoreType.DMA
    n_tok = h_norm.shape[0]
    mesh_rows = (4, 2, 2, 2)
    return pl.pallas_call(
        scatter_kernel,
        out_shape=tuple(jax.ShapeDtypeStruct(shape, jnp.float32) for shape in ((E_ROWS, 256), (W_CHUNKS, CHUNK, 256), (1, 1))),
        in_specs=[anyspace, vmem, vmem, vmem, anyspace, anyspace, anyspace, vmem],
        out_specs=(vmem,) * 3,
        scratch_shapes=[
            pltpu.VMEM((N_CHUNKS, 4, 2, 2, CHUNK, 256), jnp.float32),
            pltpu.VMEM((N_CHUNKS, 4, 2, 2, CHUNK, 256), jnp.float32),
            pltpu.VMEM((N_CHUNKS, 4, 2, HALF, 256), jnp.float32),
            pltpu.VMEM((N_CHUNKS, 4, 2, HALF, 256), jnp.float32),
            pltpu.VMEM((N_CHUNKS, 4, CHUNK, 256), jnp.float32),
            pltpu.VMEM((N_CHUNKS, 3, CHUNK, 256), jnp.float32),
            pltpu.VMEM((9, 8, 128), jnp.float32),
            pltpu.VMEM((2, *mesh_rows, CHUNK, n_tok), jnp.bfloat16),
            pltpu.VMEM((2, 4, 2, 2, CHUNK, 256), jnp.float32),
            pltpu.VMEM((512, n_tok), jnp.bfloat16),
            pltpu.VMEM((n_tok, 768), jnp.bfloat16),
            dma((W_CHUNKS,)),
            dma((2,)),
            dma((N_CHUNKS,)),
            dma((N_CHUNKS,)),
            dma((2, N_CHUNKS)),
            dma((2, N_CHUNKS)),
            dma((2, N_CHUNKS)),
            dma((2, N_CHUNKS)),
            dma((3, N_CHUNKS)),
            dma((3, N_CHUNKS)),
            dma((6,)),
            dma((6,)),
        ],
        compiler_params=pltpu.CompilerParams(collective_id=1, has_side_effects=True, vmem_limit_bytes=VMEM_LIMIT),
        name="scatter_all",
    )(d_logits_t.reshape(*mesh_rows, E_ROWS, n_tok), h_norm, grad_x, tok_ids, *(g.reshape(*mesh_rows, 64, 256) for g in (grad_gate, grad_up, grad_down)), loss_tile)


def rms_scale(rows_wide, norm_gain):
    inv_rms = lax.rsqrt(jnp.mean(rows_wide * rows_wide, axis=-1, keepdims=True) + NORM_EPS)
    return (rows_wide * inv_rms * norm_gain).astype(jnp.bfloat16), inv_rms


def rms_back(rows_wide, inv_rms, norm_gain, grad_out):
    scaled_grad = grad_out * norm_gain
    return inv_rms * (scaled_grad - rows_wide * (inv_rms * inv_rms) * jnp.mean(scaled_grad * rows_wide, axis=-1, keepdims=True))


def mlp_forward(emb_rows, gain_mlp, gain_head, w_gate, w_up, w_down):
    emb_wide = emb_rows.astype(jnp.float32)
    a_norm = rms_scale(emb_wide, gain_mlp)[0]
    gate = jnp.dot(a_norm, w_gate, preferred_element_type=jnp.float32).astype(jnp.bfloat16)
    up = jnp.dot(a_norm, w_up, preferred_element_type=jnp.float32).astype(jnp.bfloat16)
    gate_wide, up_wide = gate.astype(jnp.float32), up.astype(jnp.float32)
    gate_sig = jax.nn.sigmoid(gate_wide)
    act_rows = (gate_wide * gate_sig * up_wide).astype(jnp.bfloat16)
    hid = (emb_wide + jnp.dot(act_rows, w_down, preferred_element_type=jnp.float32)).astype(jnp.bfloat16)
    return gate, up, hid, rms_scale(hid.astype(jnp.float32), gain_head)[0]


def head_kernel(hn_ref, e_ref, lab_ref, mask_ref, n_ref, dl_ref, dhn_ref, loss_ref, ht_ref, m_s, s_s, pick_s, bias_s, coef_ref, redo):
    phase, j = pl.program_id(0), pl.program_id(1)
    n_tok = ht_ref.shape[1]
    n_tiles = pl.num_programs(1)
    vt, ur, tb = VOCAB_TILE, UNIT, TOK_TILE
    units = [(b, r) for b in range(n_tok // tb) for r in range(vt // ur)]

    def scaled(unit):
        b, r = unit
        return jnp.dot(e_ref[r * ur : (r + 1) * ur], ht_ref[:, b * tb : (b + 1) * tb], preferred_element_type=jnp.float32)

    def pipeline(process):
        ahead = scaled(units[0])
        for i, unit in enumerate(units):
            now = ahead
            if i + 1 < len(units):
                ahead = scaled(units[i + 1])
            process(unit, now.reshape(ur // 8, 8, tb))

    @pl.when(phase == 0)
    def _():
        @pl.when(j == 0)
        def _():
            ht_ref[...] = hn_ref[...].T
            coef_ref[...] = mask_ref[...].astype(jnp.float32) / n_ref[0:1, 0:1]
            m_s[...] = jnp.full_like(m_s, -jnp.inf)
            s_s[...] = jnp.zeros_like(s_s)
            pick_s[...] = jnp.zeros_like(pick_s)
            redo[0] = 1

        @pl.when(j > 0)
        def _():
            sums, tops = {}, {}

            def process(unit, t):
                b = unit[0]
                point = m_s[:, b * tb : (b + 1) * tb] * LOG2E
                part = jnp.exp2(t[0] * LOG2E - point)
                top = t[0]
                for g in range(1, ur // 8):
                    part += jnp.exp2(t[g] * LOG2E - point)
                    top = jnp.maximum(top, t[g])
                sums[b] = sums[b] + part if b in sums else part
                tops[b] = jnp.maximum(tops[b], top) if b in tops else top

            pipeline(process)
            over = jnp.max(jnp.concatenate([tops[b] - m_s[:, b * tb : (b + 1) * tb] for b in tops], axis=1))
            fits = over <= RANGE
            redo[0] = jnp.where(fits, 0, 1)
            for b in sums:
                s_s[:, b * tb : (b + 1) * tb] += jnp.where(fits, sums[b], 0.0)

        @pl.when(redo[0] == 1)
        def _():
            def process(unit, t):
                cols = pl.ds(unit[0] * tb, tb)
                m_old = m_s[:, cols]
                m_new = jnp.maximum(m_old, jnp.max(t, axis=0))
                m_s[:, cols] = m_new
                m_two = m_new * LOG2E
                s_s[:, cols] = s_s[:, cols] * jnp.exp2(m_old * LOG2E - m_two) + jnp.sum(jnp.exp2(t * LOG2E - m_two[None]), axis=0)

            pipeline(process)

        @pl.when(j == n_tiles - 1)
        def _():
            top = jnp.max(m_s[...], axis=0, keepdims=True)
            total = jnp.sum(s_s[...] * jnp.exp2((m_s[...] - top) * LOG2E), axis=0, keepdims=True)
            lse = top * LOG2E + jnp.log2(total)
            bias_s[0:1, :] = lse - jnp.log2(coef_ref[...])
            bias_s[1:2, :] = lse
            dhn_ref[...] = jnp.zeros_like(dhn_ref)

    @pl.when(phase == 1)
    def _():
        def back(b):
            cols = pl.ds(b * tb, tb)
            dhn_ref[cols, :] += lax.dot_general(dl_ref[:, cols], e_ref[...], TOK_CONTRACT, preferred_element_type=jnp.float32)

        sub = lax.broadcasted_iota(jnp.int32, (8, tb), 0)

        def process(unit, t):
            b, r = unit
            cols = pl.ds(b * tb, tb)
            if r == 0 and b > 0:
                back(b - 1)
            rel = lab_ref[:, cols] - (j * vt + r * ur) - sub
            row = lax.broadcasted_iota(jnp.int32, (ur // 8, 8, tb), 0) * 8
            is_label = row == rel[None]
            prob = jnp.exp2(t * LOG2E - bias_s[0:1, cols][None])
            dl = jnp.where(is_label, prob - coef_ref[:, cols][None], prob)
            pick = pick_s[:, cols]
            for g in range(ur // 8):
                pick = jnp.where(is_label[g], t[g], pick)
            pick_s[:, cols] = pick
            dl_ref[r * ur : (r + 1) * ur, cols] = dl.reshape(ur, tb).astype(jnp.bfloat16)

        pipeline(process)
        back(n_tok // tb - 1)

        @pl.when(j == n_tiles - 1)
        def _():
            picked = jnp.sum(pick_s[...], axis=0, keepdims=True)
            loss_ref[...] = jnp.full_like(loss_ref, jnp.sum(coef_ref[...] * (bias_s[1:2, :] * LN2 - picked)))


def head(h_norm, table, tok_labels, loss_mask, mask_total):
    n_tok, vocab = h_norm.shape[0], table.shape[0]

    def whole(*shape):
        return pl.BlockSpec(shape, lambda p, j: (0, 0))

    return pl.pallas_call(
        head_kernel,
        grid=(2, vocab // VOCAB_TILE),
        in_specs=[whole(n_tok, 256), pl.BlockSpec((VOCAB_TILE, 256), lambda p, j: (j, 0)), whole(1, n_tok), whole(1, n_tok), whole(8, 128)],
        out_specs=[pl.BlockSpec((VOCAB_TILE, n_tok), lambda p, j: (p * j, 0)), whole(n_tok, 256), whole(8, 128)],
        out_shape=(jax.ShapeDtypeStruct((vocab, n_tok), jnp.bfloat16), jax.ShapeDtypeStruct((n_tok, 256), jnp.float32), jax.ShapeDtypeStruct((8, 128), jnp.float32)),
        scratch_shapes=[pltpu.VMEM((256, n_tok), jnp.bfloat16)] + [pltpu.VMEM((8, n_tok), jnp.float32)] * 3 + [pltpu.VMEM((2, n_tok), jnp.float32), pltpu.VMEM((1, n_tok), jnp.float32), pltpu.SMEM((1,), jnp.int32)],
        compiler_params=pltpu.CompilerParams(dimension_semantics=("arbitrary", "arbitrary"), vmem_limit_bytes=VMEM_LIMIT),
        name="head",
    )(h_norm, table, tok_labels, loss_mask, mask_total)


def mlp_back_kernel(dhn_ref, h_ref, x_ref, g1_ref, g2_ref, p_ref, q_ref, wg_ref, wu_ref, wd_ref, dx_ref, gg_ref, gu_ref, gd_ref, dh_s, dhb_s, a_s, da_s):
    j = pl.program_id(0)

    @pl.when(j == 0)
    def _():
        hid_wide = h_ref[...].astype(jnp.float32)
        dh = rms_back(hid_wide, rms_scale(hid_wide, g2_ref[...])[1], g2_ref[...], dhn_ref[...])
        dh_s[...] = dh
        dhb_s[...] = dh.astype(jnp.bfloat16)
        a_s[...] = rms_scale(x_ref[...].astype(jnp.float32), g1_ref[...])[0]
        da_s[...] = jnp.zeros_like(da_s)

    dhb, a_norm = dhb_s[...], a_s[...]
    gate_wide, up_wide = p_ref[...].astype(jnp.float32), q_ref[...].astype(jnp.float32)
    gate_sig = jax.nn.sigmoid(gate_wide)
    silu = gate_wide * gate_sig
    d_act = lax.dot_general(dhb, wd_ref[...], ROW_CONTRACT, preferred_element_type=jnp.float32)
    d_up = (d_act * silu).astype(jnp.bfloat16)
    d_gate = (d_act * up_wide * gate_sig * (1.0 + gate_wide * (1.0 - gate_sig))).astype(jnp.bfloat16)
    gd_ref[...] = lax.dot_general((silu * up_wide).astype(jnp.bfloat16), dhb, TOK_CONTRACT, preferred_element_type=jnp.float32)
    gg_ref[...] = lax.dot_general(a_norm, d_gate, TOK_CONTRACT, preferred_element_type=jnp.float32)
    gu_ref[...] = lax.dot_general(a_norm, d_up, TOK_CONTRACT, preferred_element_type=jnp.float32)
    da_s[...] += lax.dot_general(d_gate, wg_ref[...], ROW_CONTRACT, preferred_element_type=jnp.float32) + lax.dot_general(d_up, wu_ref[...], ROW_CONTRACT, preferred_element_type=jnp.float32)

    @pl.when(j == pl.num_programs(0) - 1)
    def _():
        emb_wide = x_ref[...].astype(jnp.float32)
        dx_ref[...] = dh_s[...] + rms_back(emb_wide, rms_scale(emb_wide, g1_ref[...])[1], g1_ref[...], da_s[...])


def mlp_backward(d_hnorm, hid, emb_rows, gain_mlp, gain_head, gate, up, w_gate, w_up, w_down):
    n_tok, width = emb_rows.shape
    d_ff = gate.shape[1]

    def whole(*shape):
        return pl.BlockSpec(shape, lambda j: (0, 0))

    rows = whole(n_tok, width)
    gain = whole(1, width)
    tok_block = pl.BlockSpec((n_tok, FF_TILE), lambda j: (0, j))
    in_block = pl.BlockSpec((width, FF_TILE), lambda j: (0, j))
    out_block = pl.BlockSpec((FF_TILE, width), lambda j: (j, 0))
    wide = jnp.float32
    return pl.pallas_call(
        mlp_back_kernel,
        grid=(d_ff // FF_TILE,),
        in_specs=[rows, rows, rows, gain, gain, tok_block, tok_block, in_block, in_block, out_block],
        out_specs=[rows, in_block, in_block, out_block],
        out_shape=tuple(jax.ShapeDtypeStruct(shape, wide) for shape in ((n_tok, width), (width, d_ff), (width, d_ff), (d_ff, width))),
        scratch_shapes=[pltpu.VMEM((n_tok, width), kind) for kind in (wide, jnp.bfloat16, jnp.bfloat16, wide)],
        compiler_params=pltpu.CompilerParams(dimension_semantics=("arbitrary",), vmem_limit_bytes=VMEM_LIMIT),
        name="mlp_back",
    )(d_hnorm, hid, emb_rows, gain_mlp[None], gain_head[None], gate, up, w_gate, w_up, w_down)


def rows_to_tiles(rows):
    return rows.reshape(-1, 8, 8, 256).transpose(0, 2, 1, 3).reshape(-1, 64, 256)


def tiles_to_rows(tiles):
    return tiles.reshape(8, 8, 256).transpose(1, 0, 2).reshape(8, 2048)


def solution(mesh):
    def device_step(tok_ids, tok_labels, loss_mask, table_shard, gain_mlp, gain_head, gate_shard, up_shard, down_shard):
        table_blocks, gate_blocks, up_blocks, down_blocks, mask_total = gather_all(table_shard, gate_shard, up_shard, down_shard, loss_mask.reshape(8, 128))
        table_full = table_blocks.reshape(-1, 256)
        gate_full = gate_blocks.reshape(-1, 2048)
        up_full = up_blocks.reshape(-1, 2048)
        down_full = down_blocks.reshape(-1, 256)
        emb_rows = jnp.take(table_full, tok_ids, axis=0)
        gate, up, hid, h_norm = mlp_forward(emb_rows, gain_mlp, gain_head, gate_full, up_full, down_full)
        d_logits_t, d_hnorm, loss_tile = head(h_norm, table_full, tok_labels[None], loss_mask[None], mask_total)
        grad_x, grad_gate, grad_up, grad_down = mlp_backward(d_hnorm, hid, emb_rows, gain_mlp, gain_head, gate, up, gate_full, up_full, down_full)
        d_table, d_weights, loss = scatter_all(d_logits_t, h_norm, grad_x, tok_ids[None], rows_to_tiles(grad_gate), rows_to_tiles(grad_up), grad_down, loss_tile)
        d_gate, d_up, d_down = d_weights.reshape(3, 64, 256)
        return loss.reshape(()), d_table, tiles_to_rows(d_gate), tiles_to_rows(d_up), d_down

    row_spec = P("fsdp", None)
    tok_spec = P("fsdp")
    return jax.shard_map(device_step, mesh=mesh, in_specs=(tok_spec, tok_spec, tok_spec, row_spec, P(), P(), row_spec, row_spec, row_spec), out_specs=(P(), row_spec, row_spec, row_spec, row_spec), check_vma=False)
```

```python
import functools

import jax
import jax.numpy as jnp
from jax import lax
from jax.experimental import pallas as pl
from jax.experimental.pallas import tpu as pltpu
from jax.sharding import PartitionSpec as P

NORM_EPS = 1e-6
ROW_CONTRACT = (((1,), (1,)), ((), ()))
TOK_CONTRACT = (((0,), (0,)), ((), ()))
MESH = pl.DeviceIdType.MESH
N_DEV = 32
E_ROWS = 640
W_ROWS = 192
SPLIT = 416
CHUNK = 32
HALF = CHUNK // 2
E_CHUNKS = E_ROWS // CHUNK
N_CHUNKS = (E_ROWS + W_ROWS) // CHUNK
LAG = 2
AHEAD = 3
W_CHUNKS = W_ROWS // CHUNK
PER_W = 64 // CHUNK
Z_PART = 128 // CHUNK
LOG2E = 1.4426950408889634
RANGE = 40.0
LN2 = 0.6931471805599453
VOCAB_TILE = 2048
FF_TILE = 512
VMEM_LIMIT = 66060288
UNIT = 512
TOK_TILE = 256
PIECES = 7
FIRST = SPLIT // 2
ORDER = (5, 0, 1, 2, 3, 4, 6)


def dev_index(z, y, x, c):
    return z * 8 + y * 4 + x * 2 + c


def my_coords():
    me = lax.axis_index("fsdp")
    return me // 8, (me // 4) % 2, (me // 2) % 2, me % 2


def z_partners(z):
    return (z + 1 - 2 * (z % 2), (z + 2) % 4, 3 - z)


def greet(z, y, x, c):
    barrier = pltpu.get_barrier_semaphore()
    partners = [dev_index(z, y, x, 1 - c), dev_index(z, y, 1 - x, c), dev_index(z, 1 - y, x, c)]
    partners += [dev_index(zp, y, x, c) for zp in z_partners(z)]
    for dev in partners:
        pl.semaphore_signal(barrier, inc=1, device_id=(dev,), device_id_type=MESH)
    pl.semaphore_wait(barrier, 6)


def gather_kernel(e_ref, g_ref, u_ref, d_ref, mask_ref, eo_ref, go_ref, uo_ref, do_ref, n_ref, m_ref, tiles, send_sem, recv_sem, own_sem):
    z, y, x, c = my_coords()
    me = dev_index(z, y, x, c)
    zs = (z,) + z_partners(z)
    m_ref[...] = jnp.full_like(m_ref, jnp.sum(mask_ref[...].astype(jnp.float32)))
    greet(z, y, x, c)

    own_src = (e_ref.at[pl.ds(0, FIRST)], e_ref.at[pl.ds(SPLIT, E_ROWS - SPLIT)], g_ref, u_ref, d_ref, m_ref, e_ref.at[pl.ds(FIRST, FIRST)])

    def place(piece, block):
        if piece == 0:
            return eo_ref.at[block, pl.ds(0, FIRST)]
        if piece == 6:
            return eo_ref.at[block, pl.ds(FIRST, FIRST)]
        if piece == 1:
            return eo_ref.at[block, pl.ds(SPLIT, E_ROWS - SPLIT)]
        return (go_ref, uo_ref, do_ref, tiles)[piece - 2].at[block]

    sent = []
    counts = [0] * PIECES

    def send(piece, block, target, own=False):
        src = own_src[piece] if own else place(piece, block)
        copy = pltpu.make_async_remote_copy(src_ref=src, dst_ref=place(piece, block), send_sem=send_sem.at[piece, counts[piece]], recv_sem=recv_sem.at[piece, block], device_id=(target,), device_id_type=MESH)
        counts[piece] += 1
        copy.start()
        sent.append(copy)

    def arrive(piece, block):
        ref = place(piece, block)
        pltpu.make_async_copy(ref, ref, recv_sem.at[piece, block]).wait()

    to_core = dev_index(z, y, x, 1 - c)
    to_x = dev_index(z, y, 1 - x, c)
    to_y = dev_index(z, 1 - y, x, c)
    by_y, by_x = (to_y, to_x), (to_x, to_y)
    hops = (by_y, by_x, by_x, by_x, by_x, by_y, by_y)

    def block_at(piece, depth, k, j=0):
        if hops[piece] is by_y:
            ys, xs = ((y, x), (1 - y, x), ((y, 1 - y)[j], 1 - x))[depth]
        else:
            ys, xs = ((y, x), (y, 1 - x), (1 - y, (x, 1 - x)[j]))[depth]
        return dev_index(zs[k], ys, xs, c)

    for k in (1, 2, 3):
        for piece in ORDER:
            send(piece, me, dev_index(zs[k], y, x, c), own=True)
    for piece in ORDER:
        send(piece, me, hops[piece][0], own=True)
    for piece in ORDER:
        send(piece, me, hops[piece][1], own=True)
    for piece in ORDER:
        send(piece, me, to_core, own=True)
    keep = [pltpu.make_async_copy(own_src[piece], place(piece, me), own_sem.at[piece]) for piece in ORDER]
    for copy in keep:
        copy.start()

    for step in range(6):
        if 1 <= step < 4:
            for piece in ORDER:
                block = block_at(piece, 0, step)
                arrive(piece, block)
                send(piece, block, hops[piece][0])
                send(piece, block, hops[piece][1])
                send(piece, block, to_core)
        if 1 <= step < 5:
            for piece in ORDER:
                block = block_at(piece, 1, step - 1)
                arrive(piece, block)
                send(piece, block, hops[piece][1])
                send(piece, block, to_core)
        if 2 <= step < 6:
            for j in range(2):
                for piece in ORDER:
                    block = block_at(piece, 2, step - 2, j)
                    arrive(piece, block)
                    send(piece, block, to_core)
    for zb in range(4):
        for yb in range(2):
            for xb in range(2):
                for piece in ORDER:
                    arrive(piece, dev_index(zb, yb, xb, 1 - c))
    for copy in sent:
        copy.wait_send()
    for copy in keep:
        copy.wait()

    def total(i, acc):
        return acc + tiles[i]

    n_ref[...] = lax.fori_loop(0, N_DEV, total, jnp.zeros_like(n_ref))


def gather_all(e_shard, gate_shard, up_shard, down_shard, mask_tile):
    vmem = pl.BlockSpec(memory_space=pltpu.VMEM)
    anyspace = pl.BlockSpec(memory_space=pl.ANY)
    shards = (e_shard, gate_shard, up_shard, down_shard)
    return pl.pallas_call(
        gather_kernel,
        out_shape=(*(jax.ShapeDtypeStruct((N_DEV, *a.shape), a.dtype) for a in shards), jax.ShapeDtypeStruct((8, 128), jnp.float32)),
        in_specs=[vmem] * 5,
        out_specs=(*(anyspace for _ in shards), vmem),
        scratch_shapes=[
            pltpu.VMEM((8, 128), jnp.float32),
            pltpu.VMEM((N_DEV, 8, 128), jnp.float32),
            pltpu.SemaphoreType.DMA((PIECES, N_DEV)),
            pltpu.SemaphoreType.DMA((PIECES, N_DEV)),
            pltpu.SemaphoreType.DMA((PIECES,)),
        ],
        compiler_params=pltpu.CompilerParams(collective_id=0, has_side_effects=True),
        name="gather_all",
    )(*shards, mask_tile)


def scatter_kernel(dl_ref, hn_ref, dx_ref, id_ref, gg_ref, gu_ref, gd_ref, l_ref, oe_ref, ow_ref, loss_ref, acc, r0, r1a, r1b, r2, r3, bufs, dl_buf, away_buf, hot, dx_parts, own_sem, load_sem, s0, q0, s1, q1, s2, q2, s3, q3, small_send, small_recv):
    z, y, x, c = my_coords()
    to_core = dev_index(z, y, x, 1 - c)
    to_x = dev_index(z, y, 1 - x, c)
    to_y = dev_index(z, 1 - y, x, c)
    zs = z_partners(z)
    greet(z, y, x, c)

    def remote(src, dst, send_sem, recv_sem, dev):
        return pltpu.make_async_remote_copy(src_ref=src, dst_ref=dst, send_sem=send_sem, recv_sem=recv_sem, device_id=(dev,), device_id_type=MESH)

    def core_away(k, src):
        return remote(src, r0.at[k], s0.at[k], q0.at[k], to_core)

    def load(k):
        slot = k % 2
        return pltpu.make_async_copy(dl_ref.at[:, :, :, :, pl.ds((k - W_CHUNKS) * CHUNK, CHUNK)], dl_buf.at[slot], load_sem.at[slot])

    def table_rows(k):
        slot = k % 2
        load(k).wait()

        @pl.when(k >= W_CHUNKS + 2)
        def _():
            core_away(k - 2, away_buf.at[slot]).wait_send()

        row = lax.broadcasted_iota(jnp.int32, (CHUNK, id_ref.shape[1]), 0)
        hn = hn_ref[...]
        dx = dx_parts[...]
        for mine in range(2):
            core = c if mine else 1 - c

            def part(zp, carry, mine=mine, core=core):
                for i in range(4 * Z_PART):
                    dev = dev_index(Z_PART * zp + i // 4, (i // 2) % 2, i % 2, core)
                    here = row == id_ref[...] - (dev * E_ROWS + (k - W_CHUNKS) * CHUNK)
                    hot[i * CHUNK : (i + 1) * CHUNK] = jnp.where(here, 1.0, 0.0).astype(jnp.bfloat16)
                head = jnp.dot(dl_buf[slot, pl.ds(Z_PART * zp, Z_PART), :, :, core].reshape(512, -1), hn, preferred_element_type=jnp.float32)
                rows = jnp.dot(hot[...], dx, preferred_element_type=jnp.float32)
                rows = rows[:, 0:256] + (rows[:, 256:512] + rows[:, 512:768])
                total = (head + 2.0 * rows).reshape(Z_PART, 2, 2, CHUNK, 256)
                if mine:
                    acc[k, pl.ds(Z_PART * zp, Z_PART)] = total
                else:
                    away_buf[slot, pl.ds(Z_PART * zp, Z_PART)] = total
                return carry

            lax.fori_loop(0, 4 // Z_PART, part, 0)
            if not mine:
                core_away(k, away_buf.at[slot]).start()

        @pl.when(k + 2 < N_CHUNKS)
        def _():
            load(k + 2).start()

    def plane_first(k):
        return (
            remote(acc.at[k, :, :, 1 - x, pl.ds(0, HALF)], r1a.at[k], s1.at[0, k], q1.at[0, k], to_x),
            remote(acc.at[k, :, 1 - y, :, pl.ds(HALF, HALF)], r1b.at[k], s1.at[1, k], q1.at[1, k], to_y),
        )

    def plane_second(k):
        return (
            remote(r1a.at[k, :, 1 - y], r2.at[k, :, pl.ds(0, HALF)], s2.at[0, k], q2.at[0, k], to_y),
            remote(r1b.at[k, :, 1 - x], r2.at[k, :, pl.ds(HALF, HALF)], s2.at[1, k], q2.at[1, k], to_x),
        )

    def along_z(k):
        return tuple(remote(r2.at[k, zs[i]], r3.at[k, i], s3.at[i, k], q3.at[i, k], dev_index(zs[i], y, x, c)) for i in range(3))

    def small(src, slot, dev):
        return remote(src, bufs.at[slot], small_send.at[slot], small_recv.at[slot], dev)

    small_steps = (
        (small(l_ref, 0, to_core),),
        (small(bufs.at[6], 1, to_x),),
        (small(bufs.at[7], 2, to_y),),
        tuple(small(bufs.at[8], 3 + i, dev_index(zs[i], y, x, c)) for i in range(3)),
    )
    small_steps[0][0].start()
    w_refs = (gg_ref, gu_ref, gd_ref)
    for k in range(W_CHUNKS):
        rows = pl.ds(k % PER_W * CHUNK, CHUNK)
        core_away(k, w_refs[k // PER_W].at[:, :, :, 1 - c, rows]).start()
        pltpu.make_async_copy(w_refs[k // PER_W].at[:, :, :, c, rows], acc.at[k], own_sem.at[k]).start()
    for k in range(W_CHUNKS, W_CHUNKS + 2):
        load(k).start()

    def cut(i, carry):
        rows = pl.ds(pl.multiple_of(i * 128, 128), 128)
        wide = 0.5 * dx_ref[rows, :]
        for j in range(3):
            part = wide.astype(jnp.bfloat16)
            dx_parts[rows, j * 256 : (j + 1) * 256] = part
            wide = wide - part.astype(jnp.float32)
        return carry

    lax.fori_loop(0, dx_ref.shape[0] // 128, cut, 0)

    def step_body(s, carry):
        @pl.when(s < W_CHUNKS)
        def _():
            pltpu.make_async_copy(acc.at[s], acc.at[s], own_sem.at[s]).wait()

        @pl.when(s < N_CHUNKS)
        def _():
            core_away(s, r0.at[s]).wait_recv()

            def add(i, inner):
                acc[s, i // 4, (i // 2) % 2, i % 2] += r0[s, i // 4, (i // 2) % 2, i % 2]
                return inner

            lax.fori_loop(0, 16, add, 0)
            for copy in plane_first(s):
                copy.start()

        @pl.when((s >= LAG) & (s < N_CHUNKS + LAG))
        def _():
            k = s - LAG
            for copy in plane_first(k):
                copy.wait_recv()

            def add(i, inner):
                r1a[k, i // 2, i % 2] += acc[k, i // 2, i % 2, x, pl.ds(0, HALF)]
                r1b[k, i // 2, i % 2] += acc[k, i // 2, y, i % 2, pl.ds(HALF, HALF)]
                return inner

            lax.fori_loop(0, 8, add, 0)
            for copy in plane_second(k):
                copy.start()

        @pl.when((s >= 2 * LAG) & (s < N_CHUNKS + 2 * LAG))
        def _():
            k = s - 2 * LAG
            for copy in plane_second(k):
                copy.wait_recv()

            def add(i, inner):
                r2[k, i, pl.ds(0, HALF)] += r1a[k, i, y]
                r2[k, i, pl.ds(HALF, HALF)] += r1b[k, i, x]
                return inner

            lax.fori_loop(0, 4, add, 0)
            for copy in along_z(k):
                copy.start()

        @pl.when(s >= 3 * LAG)
        def _():
            k = s - 3 * LAG
            for copy in along_z(k):
                copy.wait_recv()
            total = (r2[k, z] + r3[k, 0]) + (r3[k, 1] + r3[k, 2])
            @pl.when(k < W_CHUNKS)
            def _():
                ow_ref[k] = total

            @pl.when(k >= W_CHUNKS)
            def _():
                oe_ref[pl.ds(pl.multiple_of((k - W_CHUNKS) * CHUNK, CHUNK), CHUNK)] = total

        @pl.when((s + AHEAD >= W_CHUNKS) & (s + AHEAD < N_CHUNKS))
        def _():
            table_rows(s + AHEAD)

        for i in range(3):

            @pl.when(s == 1 + 3 * i)
            def _():
                small_steps[i][0].wait()
                bufs[6 + i] = (l_ref[...] if i == 0 else bufs[5 + i]) + bufs[i]
                for copy in small_steps[i + 1]:
                    copy.start()

        return carry

    lax.fori_loop(0, N_CHUNKS + 3 * LAG, step_body, 0)

    for copy in small_steps[3]:
        copy.wait()
    loss_ref[...] = ((bufs[8] + bufs[3]) + (bufs[4] + bufs[5]))[0:1, 0:1]

    for k in (*range(W_CHUNKS), N_CHUNKS - 2, N_CHUNKS - 1):
        core_away(k, r0.at[k]).wait_send()

    def finish(k, carry):
        for copy in plane_first(k) + plane_second(k) + along_z(k):
            copy.wait_send()
        return carry

    lax.fori_loop(0, N_CHUNKS, finish, 0)


def scatter_all(d_logits_t, h_norm, grad_x, tok_ids, grad_gate, grad_up, grad_down, loss_tile):
    vmem = pl.BlockSpec(memory_space=pltpu.VMEM)
    anyspace = pl.BlockSpec(memory_space=pl.ANY)
    dma = pltpu.SemaphoreType.DMA
    n_tok = h_norm.shape[0]
    mesh_rows = (4, 2, 2, 2)
    return pl.pallas_call(
        scatter_kernel,
        out_shape=tuple(jax.ShapeDtypeStruct(shape, jnp.float32) for shape in ((E_ROWS, 256), (W_CHUNKS, CHUNK, 256), (1, 1))),
        in_specs=[anyspace, vmem, vmem, vmem, anyspace, anyspace, anyspace, vmem],
        out_specs=(vmem,) * 3,
        scratch_shapes=[
            pltpu.VMEM((N_CHUNKS, 4, 2, 2, CHUNK, 256), jnp.float32),
            pltpu.VMEM((N_CHUNKS, 4, 2, 2, CHUNK, 256), jnp.float32),
            pltpu.VMEM((N_CHUNKS, 4, 2, HALF, 256), jnp.float32),
            pltpu.VMEM((N_CHUNKS, 4, 2, HALF, 256), jnp.float32),
            pltpu.VMEM((N_CHUNKS, 4, CHUNK, 256), jnp.float32),
            pltpu.VMEM((N_CHUNKS, 3, CHUNK, 256), jnp.float32),
            pltpu.VMEM((9, 8, 128), jnp.float32),
            pltpu.VMEM((2, *mesh_rows, CHUNK, n_tok), jnp.bfloat16),
            pltpu.VMEM((2, 4, 2, 2, CHUNK, 256), jnp.float32),
            pltpu.VMEM((512, n_tok), jnp.bfloat16),
            pltpu.VMEM((n_tok, 768), jnp.bfloat16),
            dma((W_CHUNKS,)),
            dma((2,)),
            dma((N_CHUNKS,)),
            dma((N_CHUNKS,)),
            dma((2, N_CHUNKS)),
            dma((2, N_CHUNKS)),
            dma((2, N_CHUNKS)),
            dma((2, N_CHUNKS)),
            dma((3, N_CHUNKS)),
            dma((3, N_CHUNKS)),
            dma((6,)),
            dma((6,)),
        ],
        compiler_params=pltpu.CompilerParams(collective_id=1, has_side_effects=True, vmem_limit_bytes=VMEM_LIMIT),
        name="scatter_all",
    )(d_logits_t.reshape(*mesh_rows, E_ROWS, n_tok), h_norm, grad_x, tok_ids, *(g.reshape(*mesh_rows, 64, 256) for g in (grad_gate, grad_up, grad_down)), loss_tile)


def rms_scale(rows_wide, norm_gain):
    inv_rms = lax.rsqrt(jnp.mean(rows_wide * rows_wide, axis=-1, keepdims=True) + NORM_EPS)
    return (rows_wide * inv_rms * norm_gain).astype(jnp.bfloat16), inv_rms


def rms_back(rows_wide, inv_rms, norm_gain, grad_out):
    scaled_grad = grad_out * norm_gain
    return inv_rms * (scaled_grad - rows_wide * (inv_rms * inv_rms) * jnp.mean(scaled_grad * rows_wide, axis=-1, keepdims=True))


def mlp_forward(emb_rows, gain_mlp, gain_head, w_gate, w_up, w_down):
    emb_wide = emb_rows.astype(jnp.float32)
    a_norm = rms_scale(emb_wide, gain_mlp)[0]
    gate = jnp.dot(a_norm, w_gate, preferred_element_type=jnp.float32).astype(jnp.bfloat16)
    up = jnp.dot(a_norm, w_up, preferred_element_type=jnp.float32).astype(jnp.bfloat16)
    gate_wide, up_wide = gate.astype(jnp.float32), up.astype(jnp.float32)
    gate_sig = jax.nn.sigmoid(gate_wide)
    act_rows = (gate_wide * gate_sig * up_wide).astype(jnp.bfloat16)
    hid = (emb_wide + jnp.dot(act_rows, w_down, preferred_element_type=jnp.float32)).astype(jnp.bfloat16)
    return gate, up, hid, rms_scale(hid.astype(jnp.float32), gain_head)[0]


def head_kernel(hn_ref, e_ref, lab_ref, mask_ref, n_ref, dl_ref, dhn_ref, loss_ref, ht_ref, m_s, s_s, pick_s, bias_s, coef_ref, redo):
    phase, j = pl.program_id(0), pl.program_id(1)
    n_tok = ht_ref.shape[1]
    n_tiles = pl.num_programs(1)
    vt, ur, tb = VOCAB_TILE, UNIT, TOK_TILE
    units = [(b, r) for b in range(n_tok // tb) for r in range(vt // ur)]

    def scaled(unit):
        b, r = unit
        return jnp.dot(e_ref[r * ur : (r + 1) * ur], ht_ref[:, b * tb : (b + 1) * tb], preferred_element_type=jnp.float32)

    def pipeline(process):
        ahead = scaled(units[0])
        for i, unit in enumerate(units):
            now = ahead
            if i + 1 < len(units):
                ahead = scaled(units[i + 1])
            process(unit, now.reshape(ur // 8, 8, tb))

    @pl.when(phase == 0)
    def _():
        @pl.when(j == 0)
        def _():
            ht_ref[...] = hn_ref[...].T
            coef_ref[...] = mask_ref[...].astype(jnp.float32) / n_ref[0:1, 0:1]
            m_s[...] = jnp.full_like(m_s, -jnp.inf)
            s_s[...] = jnp.zeros_like(s_s)
            pick_s[...] = jnp.zeros_like(pick_s)
            redo[0] = 1

        @pl.when(j > 0)
        def _():
            sums, tops = {}, {}

            def process(unit, t):
                b = unit[0]
                point = m_s[:, b * tb : (b + 1) * tb] * LOG2E
                part = jnp.exp2(t[0] * LOG2E - point)
                top = t[0]
                for g in range(1, ur // 8):
                    part += jnp.exp2(t[g] * LOG2E - point)
                    top = jnp.maximum(top, t[g])
                sums[b] = sums[b] + part if b in sums else part
                tops[b] = jnp.maximum(tops[b], top) if b in tops else top

            pipeline(process)
            over = jnp.max(jnp.concatenate([tops[b] - m_s[:, b * tb : (b + 1) * tb] for b in tops], axis=1))
            fits = over <= RANGE
            redo[0] = jnp.where(fits, 0, 1)
            for b in sums:
                s_s[:, b * tb : (b + 1) * tb] += jnp.where(fits, sums[b], 0.0)

        @pl.when(redo[0] == 1)
        def _():
            def process(unit, t):
                cols = pl.ds(unit[0] * tb, tb)
                m_old = m_s[:, cols]
                m_new = jnp.maximum(m_old, jnp.max(t, axis=0))
                m_s[:, cols] = m_new
                m_two = m_new * LOG2E
                s_s[:, cols] = s_s[:, cols] * jnp.exp2(m_old * LOG2E - m_two) + jnp.sum(jnp.exp2(t * LOG2E - m_two[None]), axis=0)

            pipeline(process)

        @pl.when(j == n_tiles - 1)
        def _():
            top = jnp.max(m_s[...], axis=0, keepdims=True)
            total = jnp.sum(s_s[...] * jnp.exp2((m_s[...] - top) * LOG2E), axis=0, keepdims=True)
            lse = top * LOG2E + jnp.log2(total)
            bias_s[0:1, :] = lse - jnp.log2(coef_ref[...])
            bias_s[1:2, :] = lse
            dhn_ref[...] = jnp.zeros_like(dhn_ref)

    @pl.when(phase == 1)
    def _():
        def back(b):
            cols = pl.ds(b * tb, tb)
            dhn_ref[cols, :] += lax.dot_general(dl_ref[:, cols], e_ref[...], TOK_CONTRACT, preferred_element_type=jnp.float32)

        sub = lax.broadcasted_iota(jnp.int32, (8, tb), 0)

        def process(unit, t):
            b, r = unit
            cols = pl.ds(b * tb, tb)
            if r == 0 and b > 0:
                back(b - 1)
            rel = lab_ref[:, cols] - (j * vt + r * ur) - sub
            row = lax.broadcasted_iota(jnp.int32, (ur // 8, 8, tb), 0) * 8
            is_label = row == rel[None]
            prob = jnp.exp2(t * LOG2E - bias_s[0:1, cols][None])
            dl = jnp.where(is_label, prob - coef_ref[:, cols][None], prob)
            pick = pick_s[:, cols]
            for g in range(ur // 8):
                pick = jnp.where(is_label[g], t[g], pick)
            pick_s[:, cols] = pick
            dl_ref[r * ur : (r + 1) * ur, cols] = dl.reshape(ur, tb).astype(jnp.bfloat16)

        pipeline(process)
        back(n_tok // tb - 1)

        @pl.when(j == n_tiles - 1)
        def _():
            picked = jnp.sum(pick_s[...], axis=0, keepdims=True)
            loss_ref[...] = jnp.full_like(loss_ref, jnp.sum(coef_ref[...] * (bias_s[1:2, :] * LN2 - picked)))


def head(h_norm, table, tok_labels, loss_mask, mask_total):
    n_tok, vocab = h_norm.shape[0], table.shape[0]

    def whole(*shape):
        return pl.BlockSpec(shape, lambda p, j: (0, 0))

    return pl.pallas_call(
        head_kernel,
        grid=(2, vocab // VOCAB_TILE),
        in_specs=[whole(n_tok, 256), pl.BlockSpec((VOCAB_TILE, 256), lambda p, j: (j, 0)), whole(1, n_tok), whole(1, n_tok), whole(8, 128)],
        out_specs=[pl.BlockSpec((VOCAB_TILE, n_tok), lambda p, j: (p * j, 0)), whole(n_tok, 256), whole(8, 128)],
        out_shape=(jax.ShapeDtypeStruct((vocab, n_tok), jnp.bfloat16), jax.ShapeDtypeStruct((n_tok, 256), jnp.float32), jax.ShapeDtypeStruct((8, 128), jnp.float32)),
        scratch_shapes=[pltpu.VMEM((256, n_tok), jnp.bfloat16)] + [pltpu.VMEM((8, n_tok), jnp.float32)] * 3 + [pltpu.VMEM((2, n_tok), jnp.float32), pltpu.VMEM((1, n_tok), jnp.float32), pltpu.SMEM((1,), jnp.int32)],
        compiler_params=pltpu.CompilerParams(dimension_semantics=("arbitrary", "arbitrary"), vmem_limit_bytes=VMEM_LIMIT),
        name="head",
    )(h_norm, table, tok_labels, loss_mask, mask_total)


def mlp_back_kernel(dhn_ref, h_ref, x_ref, g1_ref, g2_ref, p_ref, q_ref, wg_ref, wu_ref, wd_ref, dx_ref, gg_ref, gu_ref, gd_ref, dh_s, dhb_s, a_s, da_s):
    j = pl.program_id(0)

    @pl.when(j == 0)
    def _():
        hid_wide = h_ref[...].astype(jnp.float32)
        dh = rms_back(hid_wide, rms_scale(hid_wide, g2_ref[...])[1], g2_ref[...], dhn_ref[...])
        dh_s[...] = dh
        dhb_s[...] = dh.astype(jnp.bfloat16)
        a_s[...] = rms_scale(x_ref[...].astype(jnp.float32), g1_ref[...])[0]
        da_s[...] = jnp.zeros_like(da_s)

    dhb, a_norm = dhb_s[...], a_s[...]
    gate_wide, up_wide = p_ref[...].astype(jnp.float32), q_ref[...].astype(jnp.float32)
    gate_sig = jax.nn.sigmoid(gate_wide)
    silu = gate_wide * gate_sig
    d_act = lax.dot_general(dhb, wd_ref[...], ROW_CONTRACT, preferred_element_type=jnp.float32)
    d_up = (d_act * silu).astype(jnp.bfloat16)
    d_gate = (d_act * up_wide * gate_sig * (1.0 + gate_wide * (1.0 - gate_sig))).astype(jnp.bfloat16)
    gd_ref[...] = lax.dot_general((silu * up_wide).astype(jnp.bfloat16), dhb, TOK_CONTRACT, preferred_element_type=jnp.float32)
    gg_ref[...] = lax.dot_general(a_norm, d_gate, TOK_CONTRACT, preferred_element_type=jnp.float32)
    gu_ref[...] = lax.dot_general(a_norm, d_up, TOK_CONTRACT, preferred_element_type=jnp.float32)
    da_s[...] += lax.dot_general(d_gate, wg_ref[...], ROW_CONTRACT, preferred_element_type=jnp.float32) + lax.dot_general(d_up, wu_ref[...], ROW_CONTRACT, preferred_element_type=jnp.float32)

    @pl.when(j == pl.num_programs(0) - 1)
    def _():
        emb_wide = x_ref[...].astype(jnp.float32)
        dx_ref[...] = dh_s[...] + rms_back(emb_wide, rms_scale(emb_wide, g1_ref[...])[1], g1_ref[...], da_s[...])


def mlp_backward(d_hnorm, hid, emb_rows, gain_mlp, gain_head, gate, up, w_gate, w_up, w_down):
    n_tok, width = emb_rows.shape
    d_ff = gate.shape[1]

    def whole(*shape):
        return pl.BlockSpec(shape, lambda j: (0, 0))

    rows = whole(n_tok, width)
    gain = whole(1, width)
    tok_block = pl.BlockSpec((n_tok, FF_TILE), lambda j: (0, j))
    in_block = pl.BlockSpec((width, FF_TILE), lambda j: (0, j))
    out_block = pl.BlockSpec((FF_TILE, width), lambda j: (j, 0))
    wide = jnp.float32
    return pl.pallas_call(
        mlp_back_kernel,
        grid=(d_ff // FF_TILE,),
        in_specs=[rows, rows, rows, gain, gain, tok_block, tok_block, in_block, in_block, out_block],
        out_specs=[rows, in_block, in_block, out_block],
        out_shape=tuple(jax.ShapeDtypeStruct(shape, wide) for shape in ((n_tok, width), (width, d_ff), (width, d_ff), (d_ff, width))),
        scratch_shapes=[pltpu.VMEM((n_tok, width), kind) for kind in (wide, jnp.bfloat16, jnp.bfloat16, wide)],
        compiler_params=pltpu.CompilerParams(dimension_semantics=("arbitrary",), vmem_limit_bytes=VMEM_LIMIT),
        name="mlp_back",
    )(d_hnorm, hid, emb_rows, gain_mlp[None], gain_head[None], gate, up, w_gate, w_up, w_down)


def rows_to_tiles(rows):
    return rows.reshape(-1, 8, 8, 256).transpose(0, 2, 1, 3).reshape(-1, 64, 256)


def tiles_to_rows(tiles):
    return tiles.reshape(8, 8, 256).transpose(1, 0, 2).reshape(8, 2048)


def solution(mesh):
    def device_step(tok_ids, tok_labels, loss_mask, table_shard, gain_mlp, gain_head, gate_shard, up_shard, down_shard):
        table_blocks, gate_blocks, up_blocks, down_blocks, mask_total = gather_all(table_shard, gate_shard, up_shard, down_shard, loss_mask.reshape(8, 128))
        table_full = table_blocks.reshape(-1, 256)
        gate_full = gate_blocks.reshape(-1, 2048)
        up_full = up_blocks.reshape(-1, 2048)
        down_full = down_blocks.reshape(-1, 256)
        emb_rows = jnp.take(table_full, tok_ids, axis=0)
        gate, up, hid, h_norm = mlp_forward(emb_rows, gain_mlp, gain_head, gate_full, up_full, down_full)
        d_logits_t, d_hnorm, loss_tile = head(h_norm, table_full, tok_labels[None], loss_mask[None], mask_total)
        grad_x, grad_gate, grad_up, grad_down = mlp_backward(d_hnorm, hid, emb_rows, gain_mlp, gain_head, gate, up, gate_full, up_full, down_full)
        d_table, d_weights, loss = scatter_all(d_logits_t, h_norm, grad_x, tok_ids[None], rows_to_tiles(grad_gate), rows_to_tiles(grad_up), grad_down, loss_tile)
        d_gate, d_up, d_down = d_weights.reshape(3, 64, 256)
        return loss.reshape(()), d_table, tiles_to_rows(d_gate), tiles_to_rows(d_up), d_down

    row_spec = P("fsdp", None)
    tok_spec = P("fsdp")
    return jax.shard_map(device_step, mesh=mesh, in_specs=(tok_spec, tok_spec, tok_spec, row_spec, P(), P(), row_spec, row_spec, row_spec), out_specs=(P(), row_spec, row_spec, row_spec, row_spec), check_vma=False)
```
